256 devices in a mesh: band: 128 (over z, x_lo, y, core), sub: 2 (over x_hi).
Axes of the slice: x: 4 (x_hi: 2, x_lo: 2; x = x_hi * 2 + x_lo), y: 4, z: 8, core: 2. Of those that a mesh axis runs over, the one named last changes fastest.
Arguments:
- land_values: bfloat16 [64, 4194304], P(None, ('band', 'sub')), may hold values from -6 to 6
- area_weights: bfloat16 [32768, 128, 128], P(('band', 'sub')), may hold values from 0.0019989014 to 0.029907227
- land_mask: int32 [4194304], P(('band', 'sub')), may hold values 0 or 1
- dest_band: int32 [32768, 1], P(('band', 'sub')), may hold values from 0 to 127; in each aligned block of 128 rows (0 to 127, 128 to 255, ...) at most 2 rows name the same one
- dest_tile: int32 [32768], P(('band', 'sub')), may hold values from 0 to 399
- ocean_mask: int32 [6553600], P(('band', 'sub')), may hold values 0 or 1
Outputs:
- remapped: float32 [64, 6553600], P(None, ('band', 'sub'))
The draws below stay inside these ranges and needn't reach their ends.
Inputs may be any that keep to these rules, and one draw needn't show every extreme that they name: `dest_band`: each device's 128 blocks name any one band at most 2 times; in every draw some device names one band exactly 2 times.
All inputs are finite; a program needn't handle non-finite values. No bound on the sum of `land_mask` or of `ocean_mask` on one device may be relied on, other than what follows from the above.
Results may differ from the reference program's by a relative error of at most 0.005.
Values may be sent and summed in bfloat16 or wider, within the bound.
A program may use at most 128 MiB of HBM per device.

```python
import math
import jax
import jax.numpy as jnp
import numpy as np
from jax import lax

F = 64
BL = 128
OT = 128
LB_DEV = 128
CAP = 2
TILES_BAND = 400
NBLK = 32768
NLAND = 4194304
NOCN = 6553600
N_BAND = 128


def touch_ends(result, rng, low, largest):
    longest = result.shape.index(max(result.shape))
    spots = []
    for shift in (0, 1):
        where = [jax.random.randint(jax.random.fold_in(rng, axis), (), 0, length) for axis, length in enumerate(result.shape)]
        where[longest] = (where[longest] + shift) % result.shape[longest]
        spots.append(tuple(where))
    return result.at[spots[0]].set(low).at[spots[1]].set(largest)


def level_of(stream_key, shape, split, least, largest):
    def one(position, shards_of):
        draws = jax.random.uniform(jax.random.fold_in(jax.random.fold_in(stream_key, 6), position), (shards_of,), jnp.float32, least / len(split), largest / len(split))
        return jnp.repeat(jnp.exp(draws), shape[position] // shards_of).reshape((-1,) + (1,) * (len(shape) - position - 1))

    gain = one(*split[0])
    for cut in split[1:]:
        gain = gain * one(*cut)
    return gain


def shared_out(own_key, own, number, rows, number_of, top, bound, lean):
    sequence = jax.random.permutation(own_key, number_of)
    packed, common = load_shares(number_of, rows * top, bound, lean, True), load_shares(number_of, rows * top, bound, lean, False)
    places = jnp.arange(number_of)

    def named(tallies, offset_by):
        used = int((tallies > 0).sum())
        fixed = max(1, used // 4)
        shifted = fixed + (places - fixed + offset_by * (used - fixed)) % max(1, number_of - fixed)
        return jnp.zeros((number_of,), jnp.int32).at[sequence[jnp.where(places < fixed, places, shifted)]].set(jnp.asarray(tallies, jnp.int32))

    tallies = jnp.where(number % 4 == 0, named(packed, number // 4), named(common, number - number // 4 - 1))
    mixed = jax.random.permutation(jax.random.fold_in(own, 3), number_of)
    donor, sink = mixed[0:number_of // 2 * 2:2], mixed[1:number_of // 2 * 2:2]
    room = jnp.minimum(tallies[donor] - 1, bound - tallies[sink]) // 2
    room = jnp.where((donor == sequence[0]) | (sink == sequence[0]) | (tallies[sink] == 0), 0, jnp.maximum(room, 0))
    shifted = jax.random.randint(jax.random.fold_in(own, 4), (number_of // 2,), 0, 1 << 20) % (room + 1)
    tallies = tallies.at[donor].add(-shifted).at[sink].add(shifted)
    labels = jnp.searchsorted(jnp.cumsum(tallies), jnp.arange(rows * top), side="right").astype(jnp.int32)
    listing = labels.reshape(top, rows).T
    listing = listing[jax.random.permutation(jax.random.fold_in(own, 1), rows)]
    offset_by = jax.random.randint(jax.random.fold_in(own, 2), (rows, 1), 0, top)
    return jnp.take_along_axis(listing, (jnp.arange(top)[None, :] + offset_by) % top, axis=1)


def load_shares(count, total, reach, lean, full):
    loads = [(1 << 20) // math.isqrt(rank ** lean) + 1 for rank in range(1, count + 1)]
    largest = reach if full else min(reach, max(-(-total // count), total * loads[0] // sum(loads)))
    least = 1 if total - largest >= count - 1 else 0
    given, surplus = [largest] + [least] * (count - 1), total - largest - least * (count - 1)
    while surplus > 0:
        free = [i for i in range(1, count) if given[i] < largest] or [i for i in range(1, count) if given[i] < reach]
        pool, budget = sum([loads[i] for i in free]), surplus
        for i in free:
            more = min(reach - given[i], max(1, budget * loads[i] // pool), surplus)
            given[i] = given[i] + more
            surplus = surplus - more
    return np.array(given)


def gaussian(stream_key, dims, spread, most, shards=(), dtype=jnp.bfloat16):
    drawn = jax.random.normal(stream_key, dims, jnp.float32) * spread
    if len(shards) > 0:
        drawn = level_of(stream_key, dims, shards, -0.22, 0.18) * drawn
    return jnp.clip(drawn, min=-most, max=most).astype(dtype)


def setup_inputs(seed: int = 0) -> dict:
    key_of = jax.random.split(jax.random.key(seed), 7)
    land_values = gaussian(key_of[0], (F, NLAND), 1.0, 6.0, ((1, 256),))
    area_weights = jnp.clip(jnp.exp(math.log(0.029907227) - 2.7055024 * jax.random.uniform(key_of[1], (NBLK, BL, OT), jnp.float32) ** level_of(key_of[1], (NBLK, BL, OT), ((0, 256),), -0.2, 0.2)), 0.0019989014, 0.029907227).astype(jnp.bfloat16)
    land_mask = touch_ends((jax.random.randint(key_of[2], (NLAND,), 0, 2) < 1).astype(jnp.int32), jax.random.fold_in(key_of[2], 1), 0, 1)
    dest_band_keys = jax.random.split(jax.random.fold_in(key_of[3], 1), NBLK // LB_DEV)
    dest_band_turns = jax.random.permutation(jax.random.fold_in(key_of[3], 3), NBLK // LB_DEV)
    dest_band = jax.vmap(lambda own, number: shared_out(jax.random.fold_in(key_of[3], 2), own, number, LB_DEV, N_BAND, 1, CAP, 2))(dest_band_keys, dest_band_turns).reshape((NBLK, 1))
    dest_tile = touch_ends(jax.random.randint(key_of[4], (NBLK,), 0, TILES_BAND), jax.random.fold_in(key_of[4], 1), 0, TILES_BAND - 1).astype(jnp.int32)
    ocean_mask = touch_ends((jax.random.randint(key_of[5], (NOCN,), 0, 4) < 3).astype(jnp.int32), jax.random.fold_in(key_of[5], 1), 0, 1)
    return dict(land_values=land_values, area_weights=area_weights, land_mask=land_mask, dest_band=dest_band, dest_tile=dest_tile, ocean_mask=ocean_mask)


cover_floor = 0.5


def reference(land_values, area_weights, land_mask, dest_band, dest_tile, ocean_mask):
    groups = area_weights.shape[0] // LB_DEV
    tiles_all = N_BAND * TILES_BAND
    block_values = land_values.reshape(F, groups, LB_DEV, BL).transpose(1, 2, 0, 3)
    block_weights = area_weights.reshape(groups, LB_DEV, BL, OT)
    block_masks = land_mask.reshape(groups, LB_DEV, BL)
    block_tiles = (dest_band[:, 0] * TILES_BAND + dest_tile).astype(jnp.int32).reshape(groups, LB_DEV)

    def remap_group(carry, inputs):
        summed, coverage = carry
        values, weights, masks, tiles = inputs
        masked = weights * masks.astype(jnp.bfloat16)[:, :, None]
        partial_value = jnp.einsum("bfl,blo->bfo", values.astype(jnp.float32), masked.astype(jnp.float32)).astype(jnp.bfloat16)
        covered = jnp.sum(masked.astype(jnp.float32), axis=1).astype(jnp.bfloat16)
        summed = summed.at[:, tiles].add(jnp.transpose(partial_value.astype(jnp.float32), (1, 0, 2)))
        coverage = coverage.at[tiles].add(covered.astype(jnp.float32))
        return (summed, coverage), None

    start_state = (jnp.zeros((F, tiles_all, OT), jnp.float32), jnp.zeros((tiles_all, OT), jnp.float32))
    (summed, coverage), unused = lax.scan(remap_group, start_state, (block_values, block_weights, block_masks, block_tiles))
    ocean_keep = ocean_mask.reshape(tiles_all, OT).astype(jnp.float32)
    remapped = summed * ocean_keep[None] / jnp.maximum(coverage, cover_floor)[None]
    return remapped.reshape(F, tiles_all * OT)
```

```python
import functools

import jax
import jax.numpy as jnp
from jax import lax
from jax.experimental import pallas as pl
from jax.experimental.pallas import tpu as pltpu
from jax.sharding import PartitionSpec as P

cover_floor = 0.5
MESH = pl.DeviceIdType.MESH
CAP = 2
XLO = 2
X = 4
R = 8
ROWS = 8
CODE = 32


def place():
    band, sub = lax.axis_index("band"), lax.axis_index("sub")
    z, x_lo, rem = band // (XLO * R), (band // R) % XLO, band % R
    return z, x_lo, rem, sub * XLO + x_lo


def pack_kernel(chunk, pieces, band_ref, tile_ref, values_ref, weights_ref, mask_ref, out_ref, meta_ref, count_ref):
    step = pl.program_id(0)
    z, x_lo, rem, _ = place()
    lane_base = (z * R + rem) * CAP
    lanes = lax.broadcasted_iota(jnp.int32, (1, 128), 1)

    @pl.when(step == 0)
    def _():
        meta_ref[...] = jnp.zeros_like(meta_ref)

        def clear(i, _):
            count_ref[i] = 0
            return 0

        lax.fori_loop(0, count_ref.shape[0], clear, 0)

    fields = values_ref.shape[0]
    for i in range(chunk):
        block = step * chunk + i
        band, tile = band_ref[block], tile_ref[block] + 1
        rank = count_ref[band]
        count_ref[band] = rank + 1
        peer = (band // (XLO * R)) * R + band % R
        other = jnp.where((band // R) % XLO == x_lo, 0, 1)
        keep = mask_ref[i : i + 1, :].astype(jnp.float32).astype(jnp.bfloat16)
        left = values_ref[:, i * 128 : (i + 1) * 128] * keep
        left = jnp.concatenate([left, jnp.broadcast_to(keep, (16, 128))], axis=0)
        product = jnp.dot(left, weights_ref[i], preferred_element_type=jnp.float32)
        first = other * (CAP * pieces + 1) + rank * pieces
        out_ref[peer, pl.ds(first, pieces)] = product[:fields].reshape(pieces, ROWS, 128).astype(jnp.bfloat16)
        meta_ref[peer, pl.ds(other * CAP + rank, 1), :] = product[fields : fields + 1]
        here = lanes == lane_base + rank
        high = jnp.where(here, (tile // CODE).astype(jnp.float32), 0.0)
        low = jnp.where(here, (tile % CODE).astype(jnp.float32), 0.0)
        row = 4 + other * 2
        meta_ref[peer, pl.ds(row, 1), :] += high
        meta_ref[peer, pl.ds(row + 1, 1), :] += low

    @pl.when(step == pl.num_programs(0) - 1)
    def _():
        out_ref[:, CAP * pieces] = meta_ref[...].astype(jnp.bfloat16)


def exchange_kernel(peers, pieces, send_ref, near_ref, far_ref, self_sem, send_sem, recv_sem, far_send, far_recv):
    half = CAP * pieces + 1
    planes = peers // R
    z, x_lo, rem, x = place()
    me = z * R + rem

    def yz_device(z_to, rem_to):
        return {"band": z_to * (XLO * R) + x_lo * R + rem_to, "sub": x // XLO}

    def x_device(shift):
        x_to = (x + shift) % X
        return {"band": z * (XLO * R) + (x_to % XLO) * R + rem, "sub": x_to // XLO}

    def offset(step):
        q = step // R
        dz = ((q % 2) * ((q + 1) // 2) + (1 - q % 2) * (planes - q // 2)) % planes
        return dz, step % R

    barrier = pltpu.get_barrier_semaphore()

    def greet(step, _):
        dz, dr = offset(step)
        pl.semaphore_signal(barrier, inc=1, device_id=yz_device((z + dz) % planes, (rem + dr) % R), device_id_type=MESH)
        return 0

    lax.fori_loop(1, peers, greet, 0)
    for shift in range(1, X):
        pl.semaphore_signal(barrier, inc=1, device_id=x_device(shift), device_id_type=MESH)
    own = pltpu.make_async_copy(send_ref.at[me], near_ref.at[me], self_sem)
    own.start()
    pl.semaphore_wait(barrier, peers - 1 + X - 1)

    def send(step, _):
        dz, dr = offset(step)
        z_to, rem_to = (z + dz) % planes, (rem + dr) % R
        pltpu.make_async_remote_copy(
            src_ref=send_ref.at[z_to * R + rem_to],
            dst_ref=near_ref.at[me],
            send_sem=send_sem,
            recv_sem=recv_sem.at[me],
            device_id=yz_device(z_to, rem_to),
            device_id_type=MESH,
        ).start()
        return 0

    lax.fori_loop(1, peers, send, 0)

    def forward(source):
        for way, shift in enumerate((1, X - 1, 2)):
            begin = half - 1 if way < 2 else 0
            pltpu.make_async_remote_copy(
                src_ref=near_ref.at[source, pl.ds(begin, half)],
                dst_ref=far_ref.at[way, source],
                send_sem=far_send.at[way],
                recv_sem=far_recv.at[way],
                device_id=x_device(shift),
                device_id_type=MESH,
            ).start()

    own.wait()
    forward(me)

    def relay(step, _):
        dz, dr = offset(step)
        source = ((z + planes - dz) % planes) * R + (rem + R - dr) % R
        pltpu.make_async_remote_copy(
            src_ref=send_ref.at[me],
            dst_ref=near_ref.at[source],
            send_sem=send_sem,
            recv_sem=recv_sem.at[source],
            device_id=x_device(1),
            device_id_type=MESH,
        ).wait_recv()
        forward(source)
        return 0

    lax.fori_loop(1, peers, relay, 0)
    pltpu.make_async_remote_copy(
        src_ref=send_ref.at[pl.ds(0, peers - 1)],
        dst_ref=near_ref.at[pl.ds(0, peers - 1)],
        send_sem=send_sem,
        recv_sem=recv_sem.at[0],
        device_id=x_device(1),
        device_id_type=MESH,
    ).wait_send()
    for way in range(3):
        pltpu.make_async_remote_copy(
            src_ref=far_ref.at[way],
            dst_ref=far_ref.at[way],
            send_sem=far_send.at[way],
            recv_sem=far_recv.at[way],
            device_id=x_device(1),
            device_id_type=MESH,
        ).wait()


def place_kernel(peers, pieces, near_ref, far_ref, ocean_ref, out_ref, slots, total, cover, codes, code_smem, in_sem, code_sem, out_sem):
    half = CAP * pieces + 1
    tiles = ocean_ref.shape[0]
    sub = lax.axis_index("sub")
    parts = 1 + far_ref.shape[0]
    loads = [pltpu.make_async_copy(near_ref.at[:, pl.ds(0, half)], slots.at[0], in_sem.at[0])]
    loads += [pltpu.make_async_copy(far_ref.at[w], slots.at[w + 1], in_sem.at[w + 1]) for w in range(parts - 1)]
    for load in loads:
        load.start()

    def clear(i, _):
        total[:, pl.ds(pl.multiple_of(i * 1280, 128), 1280)] = jnp.zeros((total.shape[0], 1280), jnp.float32)
        return 0

    lax.fori_loop(0, total.shape[1] // 1280, clear, 0)
    cover[...] = jnp.zeros_like(cover)
    codes[...] = jnp.zeros_like(codes)
    shape_of = [(0, half - 1, 0, 4), (1, 0, 2, 6), (1, 0, 2, 6), (0, half - 1, 0, 4)]
    for part, (_, meta, _, digit) in enumerate(shape_of):
        loads[part].wait()
        digits = jnp.sum(slots[part, :, meta].astype(jnp.float32), axis=0)
        number = digits[digit : digit + 1] * CODE + digits[digit + 1 : digit + 2]
        codes[part : part + 1, :] = number.astype(jnp.int32) - 1
    copy = pltpu.make_async_copy(codes, code_smem, code_sem)
    copy.start()
    copy.wait()
    for part, (first, meta, row, _) in enumerate(shape_of):

        def add(source, _, part=part, first=first, meta=meta, row=row):
            for k in range(CAP):
                tile = code_smem[part, source * CAP + k] - sub * tiles

                @pl.when((tile >= 0) & (tile < tiles))
                def _():
                    slot = slots[part, source, first + k * pieces : first + (k + 1) * pieces].astype(jnp.float32)
                    cells = pl.ds(pl.multiple_of(tile * 128, 128), 128)
                    total[:, cells] += slot.reshape(pieces * ROWS, 128)
                    sides = slots[part, source, meta].astype(jnp.float32)
                    cover[pl.ds(tile, 1), :] += sides[row + k : row + k + 1]

            return 0

        lax.fori_loop(0, peers, add, 0)

    group = 8
    steps = tiles // group

    def finish(i, _):
        for k in range(group):
            tile = i * group + k
            keep = ocean_ref[pl.ds(tile, 1), :].astype(jnp.float32)
            scale = keep / jnp.maximum(cover[pl.ds(tile, 1), :], cover_floor)
            cells = pl.ds(pl.multiple_of(tile * 128, 128), 128)
            total[:, cells] = total[:, cells] * scale
        cells = pl.ds(pl.multiple_of(i * group * 128, 128), group * 128)
        pltpu.make_async_copy(total.at[:, cells], out_ref.at[:, cells], out_sem).start()
        return 0

    lax.fori_loop(0, steps, finish, 0)
    pltpu.make_async_copy(total, out_ref, out_sem).wait()


def per_device(land_values, area_weights, land_mask, dest_band, dest_tile, ocean_mask):
    fields = land_values.shape[0]
    blocks, cells, tile_cells = area_weights.shape
    bands = lax.axis_size("band")
    peers = bands // XLO
    pieces = fields // ROWS
    half = CAP * pieces + 1
    tiles = ocean_mask.shape[0] // tile_cells
    chunk = 16
    send = pl.pallas_call(
        functools.partial(pack_kernel, chunk, pieces),
        grid_spec=pltpu.PrefetchScalarGridSpec(
            num_scalar_prefetch=2,
            grid=(blocks // chunk,),
            in_specs=[
                pl.BlockSpec((fields, chunk * cells), lambda s, *_: (0, s)),
                pl.BlockSpec((chunk, cells, tile_cells), lambda s, *_: (s, 0, 0)),
                pl.BlockSpec((chunk, cells), lambda s, *_: (s, 0)),
            ],
            out_specs=pl.BlockSpec((peers, 2 * half - 1, ROWS, tile_cells), lambda s, *_: (0, 0, 0, 0)),
            scratch_shapes=[
                pltpu.VMEM((peers, ROWS, tile_cells), jnp.float32),
                pltpu.SMEM((bands,), jnp.int32),
            ],
        ),
        out_shape=jax.ShapeDtypeStruct((peers, 2 * half - 1, ROWS, tile_cells), jnp.bfloat16),
        name="pack",
    )(dest_band.reshape(blocks), dest_tile, land_values, area_weights, land_mask.reshape(blocks, cells))
    near, far = pl.pallas_call(
        functools.partial(exchange_kernel, peers, pieces),
        in_specs=[pl.BlockSpec(memory_space=pl.ANY)],
        out_specs=[pl.BlockSpec(memory_space=pl.ANY)] * 2,
        out_shape=[
            jax.ShapeDtypeStruct(send.shape, jnp.bfloat16),
            jax.ShapeDtypeStruct((X - 1, peers, half, ROWS, tile_cells), jnp.bfloat16),
        ],
        scratch_shapes=[
            pltpu.SemaphoreType.DMA,
            pltpu.SemaphoreType.DMA,
            pltpu.SemaphoreType.DMA((peers,)),
            pltpu.SemaphoreType.DMA((X - 1,)),
            pltpu.SemaphoreType.DMA((X - 1,)),
        ],
        compiler_params=pltpu.CompilerParams(collective_id=0, has_side_effects=True),
        name="exchange",
    )(send)
    return pl.pallas_call(
        functools.partial(place_kernel, peers, pieces),
        in_specs=[
            pl.BlockSpec(memory_space=pl.ANY),
            pl.BlockSpec(memory_space=pl.ANY),
            pl.BlockSpec(memory_space=pltpu.VMEM),
        ],
        out_specs=pl.BlockSpec(memory_space=pl.ANY),
        out_shape=jax.ShapeDtypeStruct((fields, tiles * tile_cells), jnp.float32),
        scratch_shapes=[
            pltpu.VMEM((X, peers, half, ROWS, tile_cells), jnp.bfloat16),
            pltpu.VMEM((fields, tiles * tile_cells), jnp.float32),
            pltpu.VMEM((tiles, tile_cells), jnp.float32),
            pltpu.VMEM((8, 128), jnp.int32),
            pltpu.SMEM((8, 128), jnp.int32),
            pltpu.SemaphoreType.DMA((X,)),
            pltpu.SemaphoreType.DMA,
            pltpu.SemaphoreType.DMA,
        ],
        compiler_params=pltpu.CompilerParams(vmem_limit_bytes=40 << 20),
        name="place",
    )(near, far, ocean_mask.reshape(tiles, tile_cells))


def solution(mesh):
    in_specs = (
        P(None, ("band", "sub")),
        P(("band", "sub"), None, None),
        P(("band", "sub")),
        P(("band", "sub"), None),
        P(("band", "sub")),
        P(("band", "sub")),
    )
    return jax.shard_map(
        per_device, mesh=mesh, in_specs=in_specs, out_specs=P(None, ("band", "sub")), check_vma=False
    )
```

```python
import functools

import jax
import jax.numpy as jnp
from jax import lax
from jax.experimental import pallas as pl
from jax.experimental.pallas import tpu as pltpu
from jax.sharding import PartitionSpec as P

cover_floor = 0.5
MESH = pl.DeviceIdType.MESH
CAP = 2
XLO = 2
X = 4
R = 8
ROWS = 8
CODE = 32


def place():
    band, sub = lax.axis_index("band"), lax.axis_index("sub")
    z, x_lo, rem = band // (XLO * R), (band // R) % XLO, band % R
    return z, x_lo, rem, sub * XLO + x_lo


def pack_kernel(chunk, pieces, planes, band_ref, tile_ref, values_ref, weights_ref, mask_ref, out_ref, meta_ref, count_ref):
    step = pl.program_id(0)
    z, x_lo, rem, _ = place()
    lanes = lax.broadcasted_iota(jnp.int32, (1, 128), 1)

    @pl.when(step == 0)
    def _():
        meta_ref[...] = jnp.zeros_like(meta_ref)

        def clear(i, _):
            count_ref[i] = 0
            return 0

        lax.fori_loop(0, count_ref.shape[0], clear, 0)

    fields = values_ref.shape[0]
    for i in range(chunk):
        block = step * chunk + i
        band, tile = band_ref[block], tile_ref[block] + 1
        rank = count_ref[band]
        count_ref[band] = rank + 1
        ahead = (band // (XLO * R) + planes - z) % planes
        peer = ahead * R + band % R
        other = jnp.where((band // R) % XLO == x_lo, 0, 1)
        keep = mask_ref[i : i + 1, :].astype(jnp.float32).astype(jnp.bfloat16)
        left = values_ref[:, i * 128 : (i + 1) * 128] * keep
        left = jnp.concatenate([left, jnp.broadcast_to(keep, (16, 128))], axis=0)
        product = jnp.dot(left, weights_ref[i], preferred_element_type=jnp.float32)
        first = other * (CAP * pieces + 1) + rank * pieces
        out_ref[peer, pl.ds(first, pieces)] = product[:fields].reshape(pieces, ROWS, 128).astype(jnp.bfloat16)
        meta_ref[peer, pl.ds(other * CAP + rank, 1), :] = product[fields : fields + 1]
        here = lanes == (ahead * R + rem) * CAP + rank
        high = jnp.where(here, (tile // CODE).astype(jnp.float32), 0.0)
        low = jnp.where(here, (tile % CODE).astype(jnp.float32), 0.0)
        row = 4 + other * 2
        meta_ref[peer, pl.ds(row, 1), :] += high
        meta_ref[peer, pl.ds(row + 1, 1), :] += low

    @pl.when(step == pl.num_programs(0) - 1)
    def _():
        out_ref[:, CAP * pieces] = meta_ref[...].astype(jnp.bfloat16)


SOURCES = ((0, 0), (0, 1), (1, 0), (-1, 0), (1, 1), (-1, 1), (2, 0), (2, 1))
HOPS = [(far, hop) for far in range(1, 5) for hop in range(1, far + 1)]


def exchange_kernel(pieces, send_ref, near_ref, far_ref, held, relay, self_sem, y_send, y_recv, z_send, z_recv, x_send, x_recv):
    half = CAP * pieces + 1
    planes = near_ref.shape[0]
    z, x_lo, rem, x = place()
    y, core = rem // 2, rem % 2
    ring_y = R // 2

    def device(z_to=z, rem_to=rem, x_to=x):
        return {"band": z_to * (XLO * R) + (x_to % XLO) * R + rem_to, "sub": x_to // XLO}

    def mate(index, sign):
        dy, dc = SOURCES[index]
        return ((y + ring_y + sign * dy) % ring_y) * 2 + (core + dc) % 2

    right, left = (z + 1) % planes, (z + planes - 1) % planes
    ways = (1, X - 1, 2)

    barrier = pltpu.get_barrier_semaphore()
    greeted = [device(rem_to=mate(i, 1)) for i in range(1, R)] + [device(z_to=right), device(z_to=left)]
    greeted += [device(x_to=(x + shift) % X) for shift in ways]
    for peer in greeted:
        pl.semaphore_signal(barrier, inc=1, device_id=peer, device_id_type=MESH)
    own = [
        pltpu.make_async_copy(send_ref.at[0, rem], near_ref.at[0, rem], self_sem.at[0]),
        pltpu.make_async_copy(send_ref.at[pl.ds(1, planes - 1), rem], held.at[:, rem], self_sem.at[1]),
    ]
    for copy in own:
        copy.start()
    pl.semaphore_wait(barrier, len(greeted))

    def remote(src, dst, send_sem, recv_sem, peer):
        return pltpu.make_async_remote_copy(
            src_ref=src, dst_ref=dst, send_sem=send_sem, recv_sem=recv_sem, device_id=peer, device_id_type=MESH
        )

    def y_copy(i, onward):
        to = mate(i, 1)
        src = send_ref.at[pl.ds(1, planes - 1), to] if onward else send_ref.at[0, to]
        dst = held.at[:, rem] if onward else near_ref.at[0, rem]
        return remote(src, dst, y_send.at[onward], y_recv.at[onward, i], device(rem_to=to))

    for i in range(1, R):
        for onward in (1, 0):
            y_copy(i, onward).start()

    def forward(ahead, source):
        for way, shift in enumerate(ways):
            begin = half - 1 if way < 2 else 0
            remote(
                near_ref.at[ahead, source, pl.ds(begin, half)],
                far_ref.at[way, ahead, source],
                x_send.at[way],
                x_recv.at[way],
                device(x_to=(x + shift) % X),
            ).start()

    def travels(i, way, far):
        return far < 4 or i % 2 == way

    def z_copy(i, way, far, hop):
        source = mate(i, -1)
        at = far if way == 0 else planes - far
        slot = (far - 1) * (far - 2) // 2
        src = held.at[at - 1, source] if hop == 1 else relay.at[way, i, slot + hop - 2]
        dst = near_ref.at[at, source] if hop == far else relay.at[way, i, slot + hop - 1]
        sem = z_recv.at[way, i, HOPS.index((far, hop))]
        return remote(src, dst, z_send.at[way], sem, device(z_to=right if way == 0 else left))

    def arrive(i, way, far, hop):
        z_copy(i, way, far, hop).wait_recv()
        if hop == far:
            forward(far if way == 0 else planes - far, mate(i, -1))
        else:
            z_copy(i, way, far, hop + 1).start()

    for turn in range(R + 4):
        if turn < R:
            if turn == 0:
                own[1].wait()
            else:
                y_copy(turn, 1).wait_recv()
            for far in (1, 2, 3, 4):
                for way in (0, 1):
                    if travels(turn, way, far):
                        z_copy(turn, way, far, 1).start()
            if turn == 0:
                own[0].wait()
            else:
                y_copy(turn, 0).wait_recv()
            forward(0, mate(turn, -1))
        for hop in (4, 3, 2, 1):
            i = turn - hop
            if 0 <= i < R:
                for far in range(hop, 5):
                    for way in (0, 1):
                        if travels(i, way, far):
                            arrive(i, way, far, hop)

    remote(near_ref.at[0, pl.ds(0, R - 1)], near_ref.at[0, pl.ds(0, R - 1)], y_send.at[0], y_recv.at[0, 0], device()).wait_send()
    remote(held.at[:, pl.ds(0, R - 1)], held.at[:, pl.ds(0, R - 1)], y_send.at[1], y_recv.at[0, 0], device()).wait_send()
    for way in (0, 1):
        remote(near_ref, near_ref, z_send.at[way], y_recv.at[0, 0], device()).wait_send()
    for way in range(X - 1):
        remote(far_ref.at[way], far_ref.at[way], x_send.at[way], x_recv.at[way], device()).wait()


def place_kernel(pieces, near_ref, far_ref, ocean_ref, out_ref, total, cover, codes, code_smem, code_sem, out_sem):
    half = CAP * pieces + 1
    tiles = ocean_ref.shape[0]
    planes = near_ref.shape[0]
    sub = lax.axis_index("sub")
    parts = [((), 0, half - 1, 0, 4), ((0,), 1, 0, 2, 6), ((1,), 1, 0, 2, 6), ((2,), 0, half - 1, 0, 4)]
    refs = [near_ref] + [far_ref] * (X - 1)

    codes[...] = jnp.zeros_like(codes)
    for part, (at, _, meta, _, digit) in enumerate(parts):
        sides = refs[part][(*at, slice(None), slice(None), meta)].astype(jnp.float32)
        digits = jnp.sum(sides.reshape(planes * R, ROWS, 128), axis=0)
        number = digits[digit : digit + 1] * CODE + digits[digit + 1 : digit + 2]
        codes[part : part + 1, :] = number.astype(jnp.int32) - 1
    copy = pltpu.make_async_copy(codes, code_smem, code_sem)
    copy.start()

    def clear(i, _):
        total[:, pl.ds(pl.multiple_of(i * 1280, 128), 1280)] = jnp.zeros((total.shape[0], 1280), jnp.float32)
        return 0

    lax.fori_loop(0, total.shape[1] // 1280, clear, 0)
    cover[...] = jnp.zeros_like(cover)
    copy.wait()
    for part, (at, first, meta, row, _) in enumerate(parts):

        def add(source, _, part=part, at=at, first=first, meta=meta, row=row):
            where = (*at, source // R, source % R)
            for k in range(CAP):
                tile = code_smem[part, source * CAP + k] - sub * tiles

                @pl.when((tile >= 0) & (tile < tiles))
                def _():
                    begin = first + k * pieces
                    slot = refs[part][(*where, slice(begin, begin + pieces))].astype(jnp.float32)
                    cells = pl.ds(pl.multiple_of(tile * 128, 128), 128)
                    total[:, cells] += slot.reshape(pieces * ROWS, 128)
                    sides = refs[part][(*where, meta)].astype(jnp.float32)
                    cover[pl.ds(tile, 1), :] += sides[row + k : row + k + 1]

            return 0

        lax.fori_loop(0, planes * R, add, 0)

    group = 8
    steps = tiles // group

    def finish(i, _):
        for k in range(group):
            tile = i * group + k
            keep = ocean_ref[pl.ds(tile, 1), :].astype(jnp.float32)
            scale = keep / jnp.maximum(cover[pl.ds(tile, 1), :], cover_floor)
            cells = pl.ds(pl.multiple_of(tile * 128, 128), 128)
            total[:, cells] = total[:, cells] * scale
        cells = pl.ds(pl.multiple_of(i * group * 128, 128), group * 128)
        pltpu.make_async_copy(total.at[:, cells], out_ref.at[:, cells], out_sem).start()
        return 0

    lax.fori_loop(0, steps, finish, 0)
    pltpu.make_async_copy(total, out_ref, out_sem).wait()


def per_device(land_values, area_weights, land_mask, dest_band, dest_tile, ocean_mask):
    fields = land_values.shape[0]
    blocks, cells, tile_cells = area_weights.shape
    bands = lax.axis_size("band")
    planes = bands // (XLO * R)
    pieces = fields // ROWS
    half = CAP * pieces + 1
    tiles = ocean_mask.shape[0] // tile_cells
    chunk = 16
    unit = (2 * half - 1, ROWS, tile_cells)
    send = pl.pallas_call(
        functools.partial(pack_kernel, chunk, pieces, planes),
        grid_spec=pltpu.PrefetchScalarGridSpec(
            num_scalar_prefetch=2,
            grid=(blocks // chunk,),
            in_specs=[
                pl.BlockSpec((fields, chunk * cells), lambda s, *_: (0, s)),
                pl.BlockSpec((chunk, cells, tile_cells), lambda s, *_: (s, 0, 0)),
                pl.BlockSpec((chunk, cells), lambda s, *_: (s, 0)),
            ],
            out_specs=pl.BlockSpec((planes * R, *unit), lambda s, *_: (0, 0, 0, 0)),
            scratch_shapes=[
                pltpu.VMEM((planes * R, ROWS, tile_cells), jnp.float32),
                pltpu.SMEM((bands,), jnp.int32),
            ],
        ),
        out_shape=jax.ShapeDtypeStruct((planes * R, *unit), jnp.bfloat16),
        name="pack",
    )(dest_band.reshape(blocks), dest_tile, land_values, area_weights, land_mask.reshape(blocks, cells))
    near, far = pl.pallas_call(
        functools.partial(exchange_kernel, pieces),
        in_specs=[pl.BlockSpec(memory_space=pl.ANY)],
        out_specs=[pl.BlockSpec(memory_space=pl.ANY)] * 2,
        out_shape=[
            pltpu.VMEM((planes, R, *unit), jnp.bfloat16),
            pltpu.VMEM((X - 1, planes, R, half, ROWS, tile_cells), jnp.bfloat16),
        ],
        scratch_shapes=[
            pltpu.VMEM((planes - 1, R, *unit), jnp.bfloat16),
            pltpu.VMEM((2, R, 6, *unit), jnp.bfloat16),
            pltpu.SemaphoreType.DMA((2,)),
            pltpu.SemaphoreType.DMA((2,)),
            pltpu.SemaphoreType.DMA((2, R)),
            pltpu.SemaphoreType.DMA((2,)),
            pltpu.SemaphoreType.DMA((2, R, len(HOPS))),
            pltpu.SemaphoreType.DMA((X - 1,)),
            pltpu.SemaphoreType.DMA((X - 1,)),
        ],
        compiler_params=pltpu.CompilerParams(collective_id=0, has_side_effects=True, vmem_limit_bytes=16 << 20),
        name="exchange",
    )(send.reshape(planes, R, *unit))
    return pl.pallas_call(
        functools.partial(place_kernel, pieces),
        in_specs=[pl.BlockSpec(memory_space=pltpu.VMEM)] * 3,
        out_specs=pl.BlockSpec(memory_space=pl.ANY),
        out_shape=jax.ShapeDtypeStruct((fields, tiles * tile_cells), jnp.float32),
        scratch_shapes=[
            pltpu.VMEM((fields, tiles * tile_cells), jnp.float32),
            pltpu.VMEM((tiles, tile_cells), jnp.float32),
            pltpu.VMEM((8, 128), jnp.int32),
            pltpu.SMEM((8, 128), jnp.int32),
            pltpu.SemaphoreType.DMA,
            pltpu.SemaphoreType.DMA,
        ],
        compiler_params=pltpu.CompilerParams(vmem_limit_bytes=24 << 20),
        name="place",
    )(near, far, ocean_mask.reshape(tiles, tile_cells))


def solution(mesh):
    in_specs = (
        P(None, ("band", "sub")),
        P(("band", "sub"), None, None),
        P(("band", "sub")),
        P(("band", "sub"), None),
        P(("band", "sub")),
        P(("band", "sub")),
    )
    return jax.shard_map(
        per_device, mesh=mesh, in_specs=in_specs, out_specs=P(None, ("band", "sub")), check_vma=False
    )
```

```python
import functools

import jax
import jax.numpy as jnp
from jax import lax
from jax.experimental import pallas as pl
from jax.experimental.pallas import tpu as pltpu
from jax.sharding import PartitionSpec as P

cover_floor = 0.5
MESH = pl.DeviceIdType.MESH
CAP = 2
XLO = 2
X = 4
R = 8
ROWS = 8
CODE = 32


def place():
    band, sub = lax.axis_index("band"), lax.axis_index("sub")
    z, x_lo, rem = band // (XLO * R), (band // R) % XLO, band % R
    return z, x_lo, rem, sub * XLO + x_lo


def table_kernel(band_ref, tile_ref, out_ref):
    blocks = band_ref.shape[1]
    down = lax.broadcasted_iota(jnp.int32, (blocks, blocks), 0)
    across = lax.broadcasted_iota(jnp.int32, (blocks, blocks), 1)
    band = jnp.broadcast_to(band_ref[...], (blocks, blocks))
    tile = jnp.broadcast_to(tile_ref[...], (blocks, blocks))
    band_down = jnp.sum(jnp.where(down == across, band, 0), axis=1, keepdims=True)
    tile_down = jnp.sum(jnp.where(down == across, tile, 0), axis=1, keepdims=True) + 1
    rank_down = jnp.sum(jnp.where((band == band_down) & (across < down), 1, 0), axis=1, keepdims=True)
    slot_down = band_down * CAP + rank_down
    for part in range(CAP):
        here = slot_down == across + part * blocks
        for row, value in enumerate((down, tile_down // CODE, tile_down % CODE)):
            out_ref[row : row + 1, part * blocks : (part + 1) * blocks] = jnp.sum(
                jnp.where(here, value, 0), axis=0, keepdims=True
            )


SOURCES = ((0, 0), (0, 1), (1, 0), (-1, 0), (1, 1), (-1, 1), (2, 0), (2, 1))
HOPS = [(far, hop) for far in range(1, 5) for hop in range(1, far + 1)]


def exchange_kernel(
    pieces, table_ref, values_hbm, weights_hbm, mask_hbm, near_ref, far_ref,
    values_ref, weights_ref, mask_ref, in_sem, stage, held, relay, y_send, y_recv, z_send, z_recv, x_send, x_recv,
):
    loads = [
        pltpu.make_async_copy(weights_hbm, weights_ref, in_sem.at[1]),
        pltpu.make_async_copy(mask_hbm, mask_ref, in_sem.at[2]),
    ]
    for load in loads:
        load.start()

    def load_block(block, _):
        cells = pl.ds(pl.multiple_of(block * 128, 128), 128)
        pltpu.make_async_copy(values_hbm.at[:, cells], values_ref.at[block], in_sem.at[0]).start()
        return 0

    lax.fori_loop(0, values_ref.shape[0], load_block, 0)
    loads.append(pltpu.make_async_copy(values_ref, values_ref, in_sem.at[0]))
    half = CAP * pieces + 1
    planes = near_ref.shape[0]
    fields = values_ref.shape[1]
    z, x_lo, rem, x = place()
    y, core = rem // 2, rem % 2
    ring_y = R // 2
    row = lax.broadcasted_iota(jnp.int32, (ROWS, 128), 0)
    lane = lax.broadcasted_iota(jnp.int32, (ROWS, 128), 1)

    def device(z_to=z, rem_to=rem, x_to=x):
        return {"band": z_to * (XLO * R) + (x_to % XLO) * R + rem_to, "sub": x_to // XLO}

    def mate(index, sign):
        dy, dc = SOURCES[index]
        return ((y + ring_y + sign * dy) % ring_y) * 2 + (core + dc) % 2

    def fill(unit, ahead, to):
        start = ahead * R + rem
        sides = jnp.zeros((ROWS, 128), jnp.float32)
        for part in range(2):
            lo = x_lo if part == 0 else XLO - 1 - x_lo
            slot = (((z + ahead) % planes) * (XLO * R) + lo * R + to) * CAP
            for rank in range(CAP):
                block = table_ref[0, slot + rank]
                keep = mask_ref[block].astype(jnp.float32).astype(jnp.bfloat16)
                left = values_ref[block] * keep
                left = jnp.concatenate([left, jnp.broadcast_to(keep, (16, 128))], axis=0)
                product = jnp.dot(left, weights_ref[block], preferred_element_type=jnp.float32)
                first = part * half + rank * pieces
                unit[first : first + pieces] = product[:fields].reshape(pieces, ROWS, 128).astype(jnp.bfloat16)
                sides = jnp.where(row == part * CAP + rank, product[fields : fields + ROWS], sides)
                for digit in range(2):
                    here = (row == 4 + part * 2 + digit) & (lane == start + rank * planes * R)
                    sides = jnp.where(here, table_ref[1 + digit, slot + rank].astype(jnp.float32), sides)
        unit[half - 1] = sides.astype(jnp.bfloat16)

    def prepare(i):
        to = mate(i, 1)

        def one(ahead, _):
            fill(stage.at[i, ahead], ahead, to)
            return 0

        if i == 0:
            fill(near_ref.at[0, rem], 0, to)
            lax.fori_loop(1, planes, one, 0)
        else:
            lax.fori_loop(0, planes, one, 0)

    right, left = (z + 1) % planes, (z + planes - 1) % planes
    ways = (1, X - 1, 2)

    barrier = pltpu.get_barrier_semaphore()
    greeted = [device(rem_to=mate(i, 1)) for i in range(1, R)] + [device(z_to=right), device(z_to=left)]
    greeted += [device(x_to=(x + shift) % X) for shift in ways]
    for peer in greeted:
        pl.semaphore_signal(barrier, inc=1, device_id=peer, device_id_type=MESH)
    for load in loads:
        load.wait()
    prepare(0)
    prepare(1)
    pl.semaphore_wait(barrier, len(greeted))

    def remote(src, dst, send_sem, recv_sem, peer):
        return pltpu.make_async_remote_copy(
            src_ref=src, dst_ref=dst, send_sem=send_sem, recv_sem=recv_sem, device_id=peer, device_id_type=MESH
        )

    def y_copy(i, onward):
        to = mate(i, 1)
        src = stage.at[i, pl.ds(1, planes - 1)] if onward else stage.at[i, 0]
        dst = held.at[:, rem] if onward else near_ref.at[0, rem]
        return remote(src, dst, y_send.at[onward], y_recv.at[onward, i], device(rem_to=to))

    def y_start(i):
        for onward in (1, 0):
            y_copy(i, onward).start()

    def forward(ahead, source):
        for way, shift in enumerate(ways):
            begin = half - 1 if way < 2 else 0
            remote(
                near_ref.at[ahead, source, pl.ds(begin, half)],
                far_ref.at[way, ahead, source],
                x_send.at[way],
                x_recv.at[way],
                device(x_to=(x + shift) % X),
            ).start()

    def travels(i, way, far):
        return far < 4 or i % 2 == way

    def z_copy(i, way, far, hop):
        source = mate(i, -1)
        at = far if way == 0 else planes - far
        slot = (far - 1) * (far - 2) // 2
        first = stage.at[0, at] if i == 0 else held.at[at - 1, source]
        src = first if hop == 1 else relay.at[way, i, slot + hop - 2]
        dst = near_ref.at[at, source] if hop == far else relay.at[way, i, slot + hop - 1]
        sem = z_recv.at[way, i, HOPS.index((far, hop))]
        return remote(src, dst, z_send.at[way], sem, device(z_to=right if way == 0 else left))

    def arrive(i, way, far, hop):
        z_copy(i, way, far, hop).wait_recv()
        if hop == far:
            forward(far if way == 0 else planes - far, mate(i, -1))
        else:
            z_copy(i, way, far, hop + 1).start()

    prepared = 1
    for turn in range(R + 4):
        if turn < R:
            if turn > 0:
                y_copy(turn, 1).wait_recv()
            for far in (1, 2, 3, 4):
                for way in (0, 1):
                    if travels(turn, way, far):
                        z_copy(turn, way, far, 1).start()
            if turn > 0:
                y_copy(turn, 0).wait_recv()
            forward(0, mate(turn, -1))
        for _ in range(2 if turn < 2 else 1):
            if prepared < R:
                if prepared + 1 < R:
                    prepare(prepared + 1)
                y_start(prepared)
                prepared += 1
        for hop in (1, 2, 3, 4):
            i = turn - hop
            if 0 <= i < R:
                for far in range(hop, 5):
                    for way in (0, 1):
                        if travels(i, way, far):
                            arrive(i, way, far, hop)

    remote(near_ref.at[0, pl.ds(0, R - 1)], near_ref.at[0, pl.ds(0, R - 1)], y_send.at[0], y_recv.at[0, 0], device()).wait_send()
    remote(held.at[:, pl.ds(0, R - 1)], held.at[:, pl.ds(0, R - 1)], y_send.at[1], y_recv.at[0, 0], device()).wait_send()
    for way in (0, 1):
        remote(near_ref, near_ref, z_send.at[way], y_recv.at[0, 0], device()).wait_send()
    for way in range(X - 1):
        remote(far_ref.at[way], far_ref.at[way], x_send.at[way], x_recv.at[way], device()).wait()


def place_kernel(
    pieces, planes, near_ref, far_ref, ocean_ref, out_ref,
    total, scale, codes, code_smem, picked, code_sem, out_sem,
):
    half = CAP * pieces + 1
    tiles = ocean_ref.shape[0]
    sources = planes * R
    sub = lax.axis_index("sub")

    tile_down = lax.broadcasted_iota(jnp.int32, (tiles, sources), 0) + sub * tiles
    cover = jnp.zeros((tiles, 128), jnp.float32)
    for part in range(X):
        other = part in (1, 2)
        if part == 0:
            sides = near_ref.reshape(sources, 2 * half - 1, ROWS, 128)[:, half - 1]
        else:
            sides = far_ref.reshape(X - 1, sources, half, ROWS, 128)[part - 1, :, 0 if other else half - 1]
        sides = sides.astype(jnp.float32)
        digits = jnp.sum(sides, axis=0)
        digit = 6 if other else 4
        number = (digits[digit : digit + 1] * CODE + digits[digit + 1 : digit + 2]).astype(jnp.int32) - 1
        codes[part : part + 1, :] = number
        for rank in range(CAP):
            row = rank + (CAP if other else 0)
            chosen = tile_down == number[:, rank * sources : (rank + 1) * sources]
            chosen = jnp.where(chosen, 1.0, 0.0).astype(jnp.bfloat16)
            cover += jnp.dot(chosen, sides[:, row].astype(jnp.bfloat16), preferred_element_type=jnp.float32)
    copy = pltpu.make_async_copy(codes, code_smem, code_sem)
    copy.start()
    scale[...] = ocean_ref[...].astype(jnp.float32) / jnp.maximum(cover, cover_floor)

    def clear(i, _):
        total[:, pl.ds(pl.multiple_of(i * 1280, 128), 1280)] = jnp.zeros((total.shape[0], 1280), jnp.float32)
        return 0

    lax.fori_loop(0, tiles // 10, clear, 0)
    copy.wait()

    def pick(part, stride, offset, count):
        for rank in range(CAP):

            def one(step, count, rank=rank):
                for k in range(8):
                    source = step * 8 + k
                    tile = code_smem[part, rank * sources + source] - sub * tiles
                    start = offset + source * stride + rank * pieces
                    picked[count] = start * 256 + tile
                    count = count + jnp.where((tile >= 0) & (tile < tiles), 1, 0)
                return count

            count = lax.fori_loop(0, sources // 8, one, count)
        return count

    def add(ref, count):
        group = 4
        for k in range(group):
            picked[count + k] = tiles

        def several(step, _):
            slots = []
            for k in range(group):
                entry = picked[step * group + k]
                slot = ref[pl.ds(entry // 256, pieces)].astype(jnp.float32).reshape(pieces * ROWS, 128)
                slots.append((pl.ds(pl.multiple_of((entry % 256) * 128, 128), 128), slot))
            for cells, slot in slots:
                total[:, cells] += slot
            return 0

        lax.fori_loop(0, (count + group - 1) // group, several, 0)

    add(near_ref, pick(0, 2 * half - 1, 0, 0))
    count = pick(1, half, 1, 0)
    count = pick(2, half, sources * half + 1, count)
    add(far_ref, pick(3, half, 2 * sources * half, count))

    group = 8

    def finish(i, _):
        for k in range(group):
            tile = i * group + k
            cells = pl.ds(pl.multiple_of(tile * 128, 128), 128)
            total[:, cells] = total[:, cells] * scale[pl.ds(tile, 1), :]
        cells = pl.ds(pl.multiple_of(i * group * 128, 128), group * 128)
        pltpu.make_async_copy(total.at[:, cells], out_ref.at[:, cells], out_sem).start()
        return 0

    lax.fori_loop(0, tiles // group, finish, 0)
    pltpu.make_async_copy(total.at[:, pl.ds(0, tiles * 128)], out_ref, out_sem).wait()


def per_device(land_values, area_weights, land_mask, dest_band, dest_tile, ocean_mask):
    fields = land_values.shape[0]
    blocks, cells, tile_cells = area_weights.shape
    bands = lax.axis_size("band")
    planes = bands // (XLO * R)
    pieces = fields // ROWS
    half = CAP * pieces + 1
    tiles = ocean_mask.shape[0] // tile_cells
    unit = (2 * half - 1, ROWS, tile_cells)
    table = pl.pallas_call(
        table_kernel,
        in_specs=[pl.BlockSpec(memory_space=pltpu.VMEM)] * 2,
        out_specs=pl.BlockSpec(memory_space=pltpu.VMEM),
        out_shape=jax.ShapeDtypeStruct((3, bands * CAP), jnp.int32),
        name="table",
    )(dest_band.reshape(1, blocks), dest_tile.reshape(1, blocks))
    near, far = pl.pallas_call(
        functools.partial(exchange_kernel, pieces),
        in_specs=[
            pl.BlockSpec(memory_space=pltpu.SMEM),
            pl.BlockSpec(memory_space=pltpu.HBM),
            pl.BlockSpec(memory_space=pltpu.HBM),
            pl.BlockSpec(memory_space=pltpu.HBM),
        ],
        out_specs=[pl.BlockSpec(memory_space=pltpu.VMEM)] * 2,
        out_shape=[
            pltpu.VMEM((planes, R, *unit), jnp.bfloat16),
            pltpu.VMEM((X - 1, planes, R, half, ROWS, tile_cells), jnp.bfloat16),
        ],
        scratch_shapes=[
            pltpu.VMEM((blocks, fields, cells), jnp.bfloat16),
            pltpu.VMEM(area_weights.shape, jnp.bfloat16),
            pltpu.VMEM((blocks, 1, cells), jnp.int32),
            pltpu.SemaphoreType.DMA((3,)),
            pltpu.VMEM((R, planes, *unit), jnp.bfloat16),
            pltpu.VMEM((planes - 1, R, *unit), jnp.bfloat16),
            pltpu.VMEM((2, R, 6, *unit), jnp.bfloat16),
            pltpu.SemaphoreType.DMA((2,)),
            pltpu.SemaphoreType.DMA((2, R)),
            pltpu.SemaphoreType.DMA((2,)),
            pltpu.SemaphoreType.DMA((2, R, len(HOPS))),
            pltpu.SemaphoreType.DMA((X - 1,)),
            pltpu.SemaphoreType.DMA((X - 1,)),
        ],
        compiler_params=pltpu.CompilerParams(collective_id=0, has_side_effects=True, vmem_limit_bytes=50 << 20),
        name="exchange",
    )(table, land_values, area_weights, land_mask.reshape(blocks, 1, cells))
    near, far = near.reshape(planes * R, *unit), far.reshape(X - 1, planes * R, half, ROWS, tile_cells)
    return pl.pallas_call(
        functools.partial(place_kernel, pieces, planes),
        in_specs=[
            pl.BlockSpec(memory_space=pltpu.VMEM),
            pl.BlockSpec(memory_space=pltpu.VMEM),
            pl.BlockSpec(memory_space=pltpu.VMEM),
        ],
        out_specs=pl.BlockSpec(memory_space=pl.ANY),
        out_shape=jax.ShapeDtypeStruct((fields, tiles * tile_cells), jnp.float32),
        scratch_shapes=[
            pltpu.VMEM((fields, (tiles + 1) * tile_cells), jnp.float32),
            pltpu.VMEM((tiles, tile_cells), jnp.float32),
            pltpu.VMEM((8, 128), jnp.int32),
            pltpu.SMEM((8, 128), jnp.int32),
            pltpu.SMEM((X * CAP * planes * R + 8,), jnp.int32),
            pltpu.SemaphoreType.DMA,
            pltpu.SemaphoreType.DMA,
        ],
        compiler_params=pltpu.CompilerParams(vmem_limit_bytes=24 << 20),
        name="place",
    )(near.reshape(-1, ROWS, tile_cells), far.reshape(-1, ROWS, tile_cells), ocean_mask.reshape(tiles, tile_cells))


def solution(mesh):
    in_specs = (
        P(None, ("band", "sub")),
        P(("band", "sub"), None, None),
        P(("band", "sub")),
        P(("band", "sub"), None),
        P(("band", "sub")),
        P(("band", "sub")),
    )
    return jax.shard_map(
        per_device, mesh=mesh, in_specs=in_specs, out_specs=P(None, ("band", "sub")), check_vma=False
    )
```

```python
import functools

import jax
import jax.numpy as jnp
from jax import lax
from jax.experimental import pallas as pl
from jax.experimental.pallas import tpu as pltpu
from jax.sharding import PartitionSpec as P

cover_floor = 0.5
MESH = pl.DeviceIdType.MESH
CAP = 2
XLO = 2
X = 4
R = 8
ROWS = 8
CODE = 32


def place():
    band, sub = lax.axis_index("band"), lax.axis_index("sub")
    z, x_lo, rem = band // (XLO * R), (band // R) % XLO, band % R
    return z, x_lo, rem, sub * XLO + x_lo


def table_kernel(band_ref, tile_ref, out_ref):
    blocks = band_ref.shape[1]
    down = lax.broadcasted_iota(jnp.int32, (blocks, blocks), 0)
    across = lax.broadcasted_iota(jnp.int32, (blocks, blocks), 1)
    band = jnp.broadcast_to(band_ref[...], (blocks, blocks))
    tile = jnp.broadcast_to(tile_ref[...], (blocks, blocks))
    band_down = jnp.sum(jnp.where(down == across, band, 0), axis=1, keepdims=True)
    tile_down = jnp.sum(jnp.where(down == across, tile, 0), axis=1, keepdims=True) + 1
    rank_down = jnp.sum(jnp.where((band == band_down) & (across < down), 1, 0), axis=1, keepdims=True)
    slot_down = band_down * CAP + rank_down
    for part in range(CAP):
        here = slot_down == across + part * blocks
        for row, value in enumerate((down, tile_down // CODE, tile_down % CODE)):
            out_ref[row : row + 1, part * blocks : (part + 1) * blocks] = jnp.sum(
                jnp.where(here, value, 0), axis=0, keepdims=True
            )


SOURCES = ((0, 0), (0, 1), (1, 0), (-1, 0), (1, 1), (-1, 1), (2, 0), (2, 1))
HOPS = [(far, hop) for far in range(1, 5) for hop in range(1, far + 1)]


def exchange_kernel(
    pieces, table_ref, values_hbm, weights_hbm, mask_hbm, near_ref, far_ref,
    values_ref, weights_ref, mask_ref, in_sem, stage, held, relay, y_send, y_recv, z_send, z_recv, x_send, x_recv,
):
    loads = [
        pltpu.make_async_copy(weights_hbm, weights_ref, in_sem.at[1]),
        pltpu.make_async_copy(mask_hbm, mask_ref, in_sem.at[2]),
    ]
    for load in loads:
        load.start()

    def load_block(block, _):
        cells = pl.ds(pl.multiple_of(block * 128, 128), 128)
        pltpu.make_async_copy(values_hbm.at[:, cells], values_ref.at[block], in_sem.at[0]).start()
        return 0

    lax.fori_loop(0, values_ref.shape[0], load_block, 0)
    loads.append(pltpu.make_async_copy(values_ref, values_ref, in_sem.at[0]))
    half = CAP * pieces + 1
    planes = near_ref.shape[0]
    fields = values_ref.shape[1]
    z, x_lo, rem, x = place()
    y, core = rem // 2, rem % 2
    ring_y = R // 2
    row = lax.broadcasted_iota(jnp.int32, (ROWS, 128), 0)
    lane = lax.broadcasted_iota(jnp.int32, (ROWS, 128), 1)

    def device(z_to=z, rem_to=rem, x_to=x):
        return {"band": z_to * (XLO * R) + (x_to % XLO) * R + rem_to, "sub": x_to // XLO}

    def mate(index, sign):
        dy, dc = SOURCES[index]
        return ((y + ring_y + sign * dy) % ring_y) * 2 + (core + dc) % 2

    def fill(unit, ahead, to):
        start = ahead * R + rem
        sides = jnp.zeros((ROWS, 128), jnp.float32)
        for part in range(2):
            lo = x_lo if part == 0 else XLO - 1 - x_lo
            slot = (((z + ahead) % planes) * (XLO * R) + lo * R + to) * CAP
            for rank in range(CAP):
                block = table_ref[0, slot + rank]
                keep = mask_ref[block].astype(jnp.float32).astype(jnp.bfloat16)
                left = values_ref[block] * keep
                left = jnp.concatenate([left, jnp.broadcast_to(keep, (16, 128))], axis=0)
                product = jnp.dot(left, weights_ref[block], preferred_element_type=jnp.float32)
                first = part * half + rank * pieces
                unit[first : first + pieces] = product[:fields].reshape(pieces, ROWS, 128).astype(jnp.bfloat16)
                sides = jnp.where(row == part * CAP + rank, product[fields : fields + ROWS], sides)
                for digit in range(2):
                    here = (row == 4 + part * 2 + digit) & (lane == start + rank * planes * R)
                    sides = jnp.where(here, table_ref[1 + digit, slot + rank].astype(jnp.float32), sides)
        unit[half - 1] = sides.astype(jnp.bfloat16)

    def prepare(i):
        to = mate(i, 1)

        def one(ahead, _):
            fill(stage.at[i, ahead], ahead, to)
            return 0

        lax.fori_loop(1, planes, one, 0)

    right, left = (z + 1) % planes, (z + planes - 1) % planes
    ways = (1, X - 1, 2)

    barrier = pltpu.get_barrier_semaphore()
    greeted = [device(rem_to=mate(i, 1)) for i in range(1, R)] + [device(z_to=right), device(z_to=left)]
    greeted += [device(x_to=(x + shift) % X) for shift in ways]
    for peer in greeted:
        pl.semaphore_signal(barrier, inc=1, device_id=peer, device_id_type=MESH)
    for load in loads:
        load.wait()
    fill(near_ref.at[0, rem], 0, rem)
    for i in range(1, R):
        fill(stage.at[i, 0], 0, mate(i, 1))
    prepare(0)
    pl.semaphore_wait(barrier, len(greeted))

    def remote(src, dst, send_sem, recv_sem, peer):
        return pltpu.make_async_remote_copy(
            src_ref=src, dst_ref=dst, send_sem=send_sem, recv_sem=recv_sem, device_id=peer, device_id_type=MESH
        )

    def y_copy(i, onward):
        to = mate(i, 1)
        src = stage.at[i, pl.ds(1, planes - 1)] if onward else stage.at[i, 0]
        dst = held.at[:, rem] if onward else near_ref.at[0, rem]
        return remote(src, dst, y_send.at[onward, i], y_recv.at[onward, i], device(rem_to=to))

    def forward(ahead, source):
        for way, shift in enumerate(ways):
            begin = half - 1 if way < 2 else 0
            remote(
                near_ref.at[ahead, source, pl.ds(begin, half)],
                far_ref.at[way, ahead, source],
                x_send.at[way],
                x_recv.at[way],
                device(x_to=(x + shift) % X),
            ).start()

    def travels(i, way, far):
        return far < 4 or i % 2 == way

    def z_copy(i, way, far, hop):
        source = mate(i, -1)
        at = far if way == 0 else planes - far
        slot = (far - 1) * (far - 2) // 2
        first = stage.at[0, at] if i == 0 else held.at[at - 1, source]
        src = first if hop == 1 else relay.at[way, i, slot + hop - 2]
        dst = near_ref.at[at, source] if hop == far else relay.at[way, i, slot + hop - 1]
        sem = z_recv.at[way, i, HOPS.index((far, hop))]
        return remote(src, dst, z_send.at[way], sem, device(z_to=right if way == 0 else left))

    def arrive(i, way, far, hop):
        z_copy(i, way, far, hop).wait_recv()
        if hop == far:
            forward(far if way == 0 else planes - far, mate(i, -1))
        else:
            z_copy(i, way, far, hop + 1).start()

    def own_plane(i):
        y_copy(i, 0).wait_recv()
        forward(0, mate(i, -1))

    computed = {0: (2, 1, 3), 1: (4, 5), 3: (6, 7)}
    sent = {0: (2, 1, 3), 2: (4, 5), 4: (6,), 5: (7,)}

    def arrivals(turn):
        for hop in (1, 2, 3, 4):
            i = turn - hop
            if 0 <= i < R:
                for far in range(hop, 5):
                    for way in (0, 1):
                        if travels(i, way, far):
                            arrive(i, way, far, hop)

    for turn in range(R + 4):
        if turn == 2:
            arrivals(turn)
        if turn < R:
            if turn > 0:
                y_copy(turn, 1).wait_recv()
            for far in (1, 2, 3, 4):
                for way in (0, 1):
                    if travels(turn, way, far):
                        z_copy(turn, way, far, 1).start()
        if turn == 0:
            for i in range(1, R):
                y_copy(i, 0).start()
            forward(0, rem)
        if turn == 1:
            for i in range(1, R):
                own_plane(i)
        for i in computed.get(turn, ()):
            prepare(i)
            if i in sent.get(turn, ()):
                y_copy(i, 1).start()
        for i in sent.get(turn, ()):
            if i not in computed.get(turn, ()):
                y_copy(i - 2, 1).wait_send()
                y_copy(i, 1).start()
        if turn != 2:
            arrivals(turn)

    for i in range(1, R):
        y_copy(i, 0).wait_send()
        if i not in (2, 3, 4, 5):
            y_copy(i, 1).wait_send()
    for way in (0, 1):
        remote(near_ref, near_ref, z_send.at[way], y_recv.at[0, 0], device()).wait_send()
    for way in range(X - 1):
        remote(far_ref.at[way], far_ref.at[way], x_send.at[way], x_recv.at[way], device()).wait()


def place_kernel(
    pieces, planes, near_ref, far_ref, ocean_ref, out_ref,
    total, scale, codes, code_smem, picked, code_sem, out_sem,
):
    half = CAP * pieces + 1
    tiles = ocean_ref.shape[0]
    sources = planes * R
    sub = lax.axis_index("sub")

    tile_down = lax.broadcasted_iota(jnp.int32, (tiles, sources), 0) + sub * tiles
    cover = jnp.zeros((tiles, 128), jnp.float32)
    for part in range(X):
        other = part in (1, 2)
        if part == 0:
            sides = near_ref.reshape(sources, 2 * half - 1, ROWS, 128)[:, half - 1]
        else:
            sides = far_ref.reshape(X - 1, sources, half, ROWS, 128)[part - 1, :, 0 if other else half - 1]
        sides = sides.astype(jnp.float32)
        digits = jnp.sum(sides, axis=0)
        digit = 6 if other else 4
        number = (digits[digit : digit + 1] * CODE + digits[digit + 1 : digit + 2]).astype(jnp.int32) - 1
        codes[part : part + 1, :] = number
        for rank in range(CAP):
            row = rank + (CAP if other else 0)
            chosen = tile_down == number[:, rank * sources : (rank + 1) * sources]
            chosen = jnp.where(chosen, 1.0, 0.0).astype(jnp.bfloat16)
            cover += jnp.dot(chosen, sides[:, row].astype(jnp.bfloat16), preferred_element_type=jnp.float32)
    copy = pltpu.make_async_copy(codes, code_smem, code_sem)
    copy.start()
    scale[...] = ocean_ref[...].astype(jnp.float32) / jnp.maximum(cover, cover_floor)

    def clear(i, _):
        total[:, pl.ds(pl.multiple_of(i * 1280, 128), 1280)] = jnp.zeros((total.shape[0], 1280), jnp.float32)
        return 0

    lax.fori_loop(0, tiles // 10, clear, 0)
    copy.wait()

    def pick(part, stride, offset, count):
        for rank in range(CAP):

            def one(step, count, rank=rank):
                for k in range(8):
                    source = step * 8 + k
                    tile = code_smem[part, rank * sources + source] - sub * tiles
                    start = offset + source * stride + rank * pieces
                    picked[count] = start * 256 + tile
                    count = count + jnp.where((tile >= 0) & (tile < tiles), 1, 0)
                return count

            count = lax.fori_loop(0, sources // 8, one, count)
        return count

    def add(ref, count):
        group = 4
        for k in range(group):
            picked[count + k] = tiles

        def several(step, _):
            slots = []
            for k in range(group):
                entry = picked[step * group + k]
                slot = ref[pl.ds(entry // 256, pieces)].astype(jnp.float32).reshape(pieces * ROWS, 128)
                slots.append((pl.ds(pl.multiple_of((entry % 256) * 128, 128), 128), slot))
            for cells, slot in slots:
                total[:, cells] += slot
            return 0

        lax.fori_loop(0, (count + group - 1) // group, several, 0)

    add(near_ref, pick(0, 2 * half - 1, 0, 0))
    count = pick(1, half, 1, 0)
    count = pick(2, half, sources * half + 1, count)
    add(far_ref, pick(3, half, 2 * sources * half, count))

    group = 8

    def finish(i, _):
        for k in range(group):
            tile = i * group + k
            cells = pl.ds(pl.multiple_of(tile * 128, 128), 128)
            total[:, cells] = total[:, cells] * scale[pl.ds(tile, 1), :]
        cells = pl.ds(pl.multiple_of(i * group * 128, 128), group * 128)
        pltpu.make_async_copy(total.at[:, cells], out_ref.at[:, cells], out_sem).start()
        return 0

    lax.fori_loop(0, tiles // group, finish, 0)
    pltpu.make_async_copy(total.at[:, pl.ds(0, tiles * 128)], out_ref, out_sem).wait()


def per_device(land_values, area_weights, land_mask, dest_band, dest_tile, ocean_mask):
    fields = land_values.shape[0]
    blocks, cells, tile_cells = area_weights.shape
    bands = lax.axis_size("band")
    planes = bands // (XLO * R)
    pieces = fields // ROWS
    half = CAP * pieces + 1
    tiles = ocean_mask.shape[0] // tile_cells
    unit = (2 * half - 1, ROWS, tile_cells)
    table = pl.pallas_call(
        table_kernel,
        in_specs=[pl.BlockSpec(memory_space=pltpu.VMEM)] * 2,
        out_specs=pl.BlockSpec(memory_space=pltpu.VMEM),
        out_shape=jax.ShapeDtypeStruct((3, bands * CAP), jnp.int32),
        name="table",
    )(dest_band.reshape(1, blocks), dest_tile.reshape(1, blocks))
    near, far = pl.pallas_call(
        functools.partial(exchange_kernel, pieces),
        in_specs=[
            pl.BlockSpec(memory_space=pltpu.SMEM),
            pl.BlockSpec(memory_space=pltpu.HBM),
            pl.BlockSpec(memory_space=pltpu.HBM),
            pl.BlockSpec(memory_space=pltpu.HBM),
        ],
        out_specs=[pl.BlockSpec(memory_space=pltpu.VMEM)] * 2,
        out_shape=[
            pltpu.VMEM((planes, R, *unit), jnp.bfloat16),
            pltpu.VMEM((X - 1, planes, R, half, ROWS, tile_cells), jnp.bfloat16),
        ],
        scratch_shapes=[
            pltpu.VMEM((blocks, fields, cells), jnp.bfloat16),
            pltpu.VMEM(area_weights.shape, jnp.bfloat16),
            pltpu.VMEM((blocks, 1, cells), jnp.int32),
            pltpu.SemaphoreType.DMA((3,)),
            pltpu.VMEM((R, planes, *unit), jnp.bfloat16),
            pltpu.VMEM((planes - 1, R, *unit), jnp.bfloat16),
            pltpu.VMEM((2, R, 6, *unit), jnp.bfloat16),
            pltpu.SemaphoreType.DMA((2, R)),
            pltpu.SemaphoreType.DMA((2, R)),
            pltpu.SemaphoreType.DMA((2,)),
            pltpu.SemaphoreType.DMA((2, R, len(HOPS))),
            pltpu.SemaphoreType.DMA((X - 1,)),
            pltpu.SemaphoreType.DMA((X - 1,)),
        ],
        compiler_params=pltpu.CompilerParams(collective_id=0, has_side_effects=True, vmem_limit_bytes=50 << 20),
        name="exchange",
    )(table, land_values, area_weights, land_mask.reshape(blocks, 1, cells))
    near, far = near.reshape(planes * R, *unit), far.reshape(X - 1, planes * R, half, ROWS, tile_cells)
    return pl.pallas_call(
        functools.partial(place_kernel, pieces, planes),
        in_specs=[
            pl.BlockSpec(memory_space=pltpu.VMEM),
            pl.BlockSpec(memory_space=pltpu.VMEM),
            pl.BlockSpec(memory_space=pltpu.VMEM),
        ],
        out_specs=pl.BlockSpec(memory_space=pl.ANY),
        out_shape=jax.ShapeDtypeStruct((fields, tiles * tile_cells), jnp.float32),
        scratch_shapes=[
            pltpu.VMEM((fields, (tiles + 1) * tile_cells), jnp.float32),
            pltpu.VMEM((tiles, tile_cells), jnp.float32),
            pltpu.VMEM((8, 128), jnp.int32),
            pltpu.SMEM((8, 128), jnp.int32),
            pltpu.SMEM((X * CAP * planes * R + 8,), jnp.int32),
            pltpu.SemaphoreType.DMA,
            pltpu.SemaphoreType.DMA,
        ],
        compiler_params=pltpu.CompilerParams(vmem_limit_bytes=24 << 20),
        name="place",
    )(near.reshape(-1, ROWS, tile_cells), far.reshape(-1, ROWS, tile_cells), ocean_mask.reshape(tiles, tile_cells))


def solution(mesh):
    in_specs = (
        P(None, ("band", "sub")),
        P(("band", "sub"), None, None),
        P(("band", "sub")),
        P(("band", "sub"), None),
        P(("band", "sub")),
        P(("band", "sub")),
    )
    return jax.shard_map(
        per_device, mesh=mesh, in_specs=in_specs, out_specs=P(None, ("band", "sub")), check_vma=False
    )
```

```python
import functools

import jax
import jax.numpy as jnp
from jax import lax
from jax.experimental import pallas as pl
from jax.experimental.pallas import tpu as pltpu
from jax.sharding import PartitionSpec as P

cover_floor = 0.5
MESH = pl.DeviceIdType.MESH
CAP = 2
XLO = 2
X = 4
R = 8
ROWS = 8
CODE = 32


def place():
    band, sub = lax.axis_index("band"), lax.axis_index("sub")
    z, x_lo, rem = band // (XLO * R), (band // R) % XLO, band % R
    return z, x_lo, rem, sub * XLO + x_lo


def make_table(band_ref, tile_ref, out_ref):
    blocks = band_ref.shape[1]
    down = lax.broadcasted_iota(jnp.int32, (blocks, blocks), 0)
    across = lax.broadcasted_iota(jnp.int32, (blocks, blocks), 1)
    out_ref[...] = jnp.zeros_like(out_ref)
    band = jnp.broadcast_to(band_ref[...], (blocks, blocks))
    tile = jnp.broadcast_to(tile_ref[...], (blocks, blocks))
    band_down = jnp.sum(jnp.where(down == across, band, 0), axis=1, keepdims=True)
    tile_down = jnp.sum(jnp.where(down == across, tile, 0), axis=1, keepdims=True) + 1
    rank_down = jnp.sum(jnp.where((band == band_down) & (across < down), 1, 0), axis=1, keepdims=True)
    slot_down = band_down * CAP + rank_down
    for part in range(CAP):
        here = slot_down == across + part * blocks
        for row, value in enumerate((down, tile_down // CODE, tile_down % CODE)):
            out_ref[row : row + 1, part * blocks : (part + 1) * blocks] = jnp.sum(
                jnp.where(here, value, 0), axis=0, keepdims=True
            )


SOURCES = ((0, 0), (0, 1), (1, 0), (-1, 0), (1, 1), (-1, 1), (2, 0), (2, 1))
HOPS = [(far, hop) for far in range(1, 5) for hop in range(1, far + 1)]


def exchange_kernel(
    pieces, band_hbm, tile_hbm, values_hbm, weights_hbm, mask_hbm, near_ref, far_ref,
    band_ref, tile_ref, table_vmem, table_ref, values_ref, weights_ref, mask_ref, in_sem, stage, held, relay, y_send, y_recv, z_send, z_recv, x_send, x_recv,
):
    names = [
        pltpu.make_async_copy(band_hbm, band_ref, in_sem.at[3]),
        pltpu.make_async_copy(tile_hbm, tile_ref, in_sem.at[4]),
    ]
    loads = [
        pltpu.make_async_copy(weights_hbm, weights_ref, in_sem.at[1]),
        pltpu.make_async_copy(mask_hbm, mask_ref, in_sem.at[2]),
    ]
    for load in names + loads:
        load.start()

    def load_block(block, _):
        cells = pl.ds(pl.multiple_of(block * 128, 128), 128)
        pltpu.make_async_copy(values_hbm.at[:, cells], values_ref.at[block], in_sem.at[0]).start()
        return 0

    lax.fori_loop(0, values_ref.shape[0], load_block, 0)
    loads.append(pltpu.make_async_copy(values_ref, values_ref, in_sem.at[0]))
    half = CAP * pieces + 1
    planes = near_ref.shape[0]
    fields = values_ref.shape[1]
    z, x_lo, rem, x = place()
    y, core = rem // 2, rem % 2
    ring_y = R // 2
    row = lax.broadcasted_iota(jnp.int32, (ROWS, 128), 0)
    lane = lax.broadcasted_iota(jnp.int32, (ROWS, 128), 1)

    def device(z_to=z, rem_to=rem, x_to=x):
        return {"band": z_to * (XLO * R) + (x_to % XLO) * R + rem_to, "sub": x_to // XLO}

    def mate(index, sign):
        dy, dc = SOURCES[index]
        return ((y + ring_y + sign * dy) % ring_y) * 2 + (core + dc) % 2

    def fill(unit, ahead, to):
        start = ahead * R + rem
        sides = jnp.zeros((ROWS, 128), jnp.float32)
        for part in range(2):
            lo = x_lo if part == 0 else XLO - 1 - x_lo
            slot = (((z + ahead) % planes) * (XLO * R) + lo * R + to) * CAP
            for rank in range(CAP):
                block = table_ref[0, slot + rank]
                keep = mask_ref[block].astype(jnp.float32).astype(jnp.bfloat16)
                left = values_ref[block] * keep
                left = jnp.concatenate([left, jnp.broadcast_to(keep, (16, 128))], axis=0)
                product = jnp.dot(left, weights_ref[block], preferred_element_type=jnp.float32)
                first = part * half + rank * pieces
                unit[first : first + pieces] = product[:fields].reshape(pieces, ROWS, 128).astype(jnp.bfloat16)
                sides = jnp.where(row == part * CAP + rank, product[fields : fields + ROWS], sides)
                for digit in range(2):
                    here = (row == 4 + part * 2 + digit) & (lane == start + rank * planes * R)
                    sides = jnp.where(here, table_ref[1 + digit, slot + rank].astype(jnp.float32), sides)
        unit[half - 1] = sides.astype(jnp.bfloat16)

    def prepare(i):
        to = mate(i, 1)

        def one(ahead, _):
            fill(stage.at[i, ahead], ahead, to)
            return 0

        lax.fori_loop(1, planes, one, 0)

    right, left = (z + 1) % planes, (z + planes - 1) % planes
    ways = (1, X - 1, 2)

    barrier = pltpu.get_barrier_semaphore()
    greeted = [device(rem_to=mate(i, 1)) for i in range(1, R)] + [device(z_to=right), device(z_to=left)]
    greeted += [device(x_to=(x + shift) % X) for shift in ways]
    for peer in greeted:
        pl.semaphore_signal(barrier, inc=1, device_id=peer, device_id_type=MESH)
    for load in names:
        load.wait()
    make_table(band_ref, tile_ref, table_vmem)
    loads.append(pltpu.make_async_copy(table_vmem, table_ref, in_sem.at[5]))
    loads[-1].start()
    for load in loads:
        load.wait()
    fill(near_ref.at[0, rem], 0, rem)
    for i in range(1, R):
        fill(stage.at[i, 0], 0, mate(i, 1))
    prepare(0)
    pl.semaphore_wait(barrier, len(greeted))

    def remote(src, dst, send_sem, recv_sem, peer):
        return pltpu.make_async_remote_copy(
            src_ref=src, dst_ref=dst, send_sem=send_sem, recv_sem=recv_sem, device_id=peer, device_id_type=MESH
        )

    def y_copy(i, onward):
        to = mate(i, 1)
        src = stage.at[i, pl.ds(1, planes - 1)] if onward else stage.at[i, 0]
        dst = held.at[:, rem] if onward else near_ref.at[0, rem]
        return remote(src, dst, y_send.at[onward, i], y_recv.at[onward, i], device(rem_to=to))

    def forward(ahead, source):
        for way, shift in enumerate(ways):
            begin = half - 1 if way < 2 else 0
            remote(
                near_ref.at[ahead, source, pl.ds(begin, half)],
                far_ref.at[way, ahead, source],
                x_send.at[way],
                x_recv.at[way],
                device(x_to=(x + shift) % X),
            ).start()

    def travels(i, way, far):
        return far < 4 or i % 2 == way

    def z_copy(i, way, far, hop):
        source = mate(i, -1)
        at = far if way == 0 else planes - far
        slot = (far - 1) * (far - 2) // 2
        first = stage.at[0, at] if i == 0 else held.at[at - 1, source]
        src = first if hop == 1 else relay.at[way, i, slot + hop - 2]
        dst = near_ref.at[at, source] if hop == far else relay.at[way, i, slot + hop - 1]
        sem = z_recv.at[way, i, HOPS.index((far, hop))]
        return remote(src, dst, z_send.at[way], sem, device(z_to=right if way == 0 else left))

    def arrive(i, way, far, hop):
        z_copy(i, way, far, hop).wait_recv()
        if hop == far:
            forward(far if way == 0 else planes - far, mate(i, -1))
        else:
            z_copy(i, way, far, hop + 1).start()

    def own_plane(i):
        y_copy(i, 0).wait_recv()
        forward(0, mate(i, -1))

    computed = {0: (2, 1, 3), 1: (4, 5), 3: (6, 7)}
    sent = {0: (2, 1, 3), 2: (4, 5), 4: (6,), 5: (7,)}

    def arrivals(turn):
        for hop in (1, 2, 3, 4):
            i = turn - hop
            if 0 <= i < R:
                for far in range(hop, 5):
                    for way in (0, 1):
                        if travels(i, way, far):
                            arrive(i, way, far, hop)

    for turn in range(R + 4):
        if turn == 2:
            arrivals(turn)
        if turn < R:
            if turn > 0:
                y_copy(turn, 1).wait_recv()
            for far in (1, 2, 3, 4):
                for way in (0, 1):
                    if travels(turn, way, far):
                        z_copy(turn, way, far, 1).start()
        if turn == 0:
            for i in range(1, R):
                y_copy(i, 0).start()
            forward(0, rem)
        if turn == 1:
            for i in range(1, R):
                own_plane(i)
        for i in computed.get(turn, ()):
            prepare(i)
            if i in sent.get(turn, ()):
                y_copy(i, 1).start()
        for i in sent.get(turn, ()):
            if i not in computed.get(turn, ()):
                y_copy(i - 2, 1).wait_send()
                y_copy(i, 1).start()
        if turn != 2:
            arrivals(turn)

    for i in range(1, R):
        y_copy(i, 0).wait_send()
        if i not in (2, 3, 4, 5):
            y_copy(i, 1).wait_send()
    for way in (0, 1):
        remote(near_ref, near_ref, z_send.at[way], y_recv.at[0, 0], device()).wait_send()
    for way in range(X - 1):
        remote(far_ref.at[way], far_ref.at[way], x_send.at[way], x_recv.at[way], device()).wait()


def place_kernel(
    pieces, planes, near_ref, far_ref, ocean_ref, out_ref,
    total, scale, codes, code_smem, picked, code_sem, out_sem,
):
    half = CAP * pieces + 1
    tiles = ocean_ref.shape[0]
    sources = planes * R
    sub = lax.axis_index("sub")

    tile_down = lax.broadcasted_iota(jnp.int32, (tiles, sources), 0) + sub * tiles
    cover = jnp.zeros((tiles, 128), jnp.float32)
    for part in range(X):
        other = part in (1, 2)
        if part == 0:
            sides = near_ref.reshape(sources, 2 * half - 1, ROWS, 128)[:, half - 1]
        else:
            sides = far_ref.reshape(X - 1, sources, half, ROWS, 128)[part - 1, :, 0 if other else half - 1]
        sides = sides.astype(jnp.float32)
        digits = jnp.sum(sides, axis=0)
        digit = 6 if other else 4
        number = (digits[digit : digit + 1] * CODE + digits[digit + 1 : digit + 2]).astype(jnp.int32) - 1
        codes[part : part + 1, :] = number
        for rank in range(CAP):
            row = rank + (CAP if other else 0)
            chosen = tile_down == number[:, rank * sources : (rank + 1) * sources]
            chosen = jnp.where(chosen, 1.0, 0.0).astype(jnp.bfloat16)
            cover += jnp.dot(chosen, sides[:, row].astype(jnp.bfloat16), preferred_element_type=jnp.float32)
    copy = pltpu.make_async_copy(codes, code_smem, code_sem)
    copy.start()
    scale[...] = ocean_ref[...].astype(jnp.float32) / jnp.maximum(cover, cover_floor)

    def clear(i, _):
        total[:, pl.ds(pl.multiple_of(i * 1280, 128), 1280)] = jnp.zeros((total.shape[0], 1280), jnp.float32)
        return 0

    lax.fori_loop(0, tiles // 10, clear, 0)
    copy.wait()

    def pick(part, stride, offset, count):
        for rank in range(CAP):

            def one(step, count, rank=rank):
                for k in range(8):
                    source = step * 8 + k
                    tile = code_smem[part, rank * sources + source] - sub * tiles
                    start = offset + source * stride + rank * pieces
                    picked[count] = start * 256 + tile
                    count = count + jnp.where((tile >= 0) & (tile < tiles), 1, 0)
                return count

            count = lax.fori_loop(0, sources // 8, one, count)
        return count

    def add(ref, count):
        group = 4
        for k in range(group):
            picked[count + k] = tiles

        def several(step, _):
            slots = []
            for k in range(group):
                entry = picked[step * group + k]
                slot = ref[pl.ds(entry // 256, pieces)].astype(jnp.float32).reshape(pieces * ROWS, 128)
                slots.append((pl.ds(pl.multiple_of((entry % 256) * 128, 128), 128), slot))
            for cells, slot in slots:
                total[:, cells] += slot
            return 0

        lax.fori_loop(0, (count + group - 1) // group, several, 0)

    add(near_ref, pick(0, 2 * half - 1, 0, 0))
    count = pick(1, half, 1, 0)
    count = pick(2, half, sources * half + 1, count)
    add(far_ref, pick(3, half, 2 * sources * half, count))

    group = 8

    def finish(i, _):
        for k in range(group):
            tile = i * group + k
            cells = pl.ds(pl.multiple_of(tile * 128, 128), 128)
            total[:, cells] = total[:, cells] * scale[pl.ds(tile, 1), :]
        cells = pl.ds(pl.multiple_of(i * group * 128, 128), group * 128)
        pltpu.make_async_copy(total.at[:, cells], out_ref.at[:, cells], out_sem).start()
        return 0

    lax.fori_loop(0, tiles // group, finish, 0)
    pltpu.make_async_copy(total.at[:, pl.ds(0, tiles * 128)], out_ref, out_sem).wait()


def per_device(land_values, area_weights, land_mask, dest_band, dest_tile, ocean_mask):
    fields = land_values.shape[0]
    blocks, cells, tile_cells = area_weights.shape
    bands = lax.axis_size("band")
    planes = bands // (XLO * R)
    pieces = fields // ROWS
    half = CAP * pieces + 1
    tiles = ocean_mask.shape[0] // tile_cells
    unit = (2 * half - 1, ROWS, tile_cells)
    near, far = pl.pallas_call(
        functools.partial(exchange_kernel, pieces),
        in_specs=[pl.BlockSpec(memory_space=pltpu.HBM)] * 5,
        out_specs=[pl.BlockSpec(memory_space=pltpu.VMEM)] * 2,
        out_shape=[
            pltpu.VMEM((planes, R, *unit), jnp.bfloat16),
            pltpu.VMEM((X - 1, planes, R, half, ROWS, tile_cells), jnp.bfloat16),
        ],
        scratch_shapes=[
            pltpu.VMEM((1, blocks), jnp.int32),
            pltpu.VMEM((1, blocks), jnp.int32),
            pltpu.VMEM((8, bands * CAP), jnp.int32),
            pltpu.SMEM((8, bands * CAP), jnp.int32),
            pltpu.VMEM((blocks, fields, cells), jnp.bfloat16),
            pltpu.VMEM(area_weights.shape, jnp.bfloat16),
            pltpu.VMEM((blocks, 1, cells), jnp.int32),
            pltpu.SemaphoreType.DMA((6,)),
            pltpu.VMEM((R, planes, *unit), jnp.bfloat16),
            pltpu.VMEM((planes - 1, R, *unit), jnp.bfloat16),
            pltpu.VMEM((2, R, 6, *unit), jnp.bfloat16),
            pltpu.SemaphoreType.DMA((2, R)),
            pltpu.SemaphoreType.DMA((2, R)),
            pltpu.SemaphoreType.DMA((2,)),
            pltpu.SemaphoreType.DMA((2, R, len(HOPS))),
            pltpu.SemaphoreType.DMA((X - 1,)),
            pltpu.SemaphoreType.DMA((X - 1,)),
        ],
        compiler_params=pltpu.CompilerParams(collective_id=0, has_side_effects=True, vmem_limit_bytes=50 << 20),
        name="exchange",
    )(
        dest_band.reshape(1, blocks),
        dest_tile.reshape(1, blocks),
        land_values,
        area_weights,
        land_mask.reshape(blocks, 1, cells),
    )
    near, far = near.reshape(planes * R, *unit), far.reshape(X - 1, planes * R, half, ROWS, tile_cells)
    return pl.pallas_call(
        functools.partial(place_kernel, pieces, planes),
        in_specs=[
            pl.BlockSpec(memory_space=pltpu.VMEM),
            pl.BlockSpec(memory_space=pltpu.VMEM),
            pl.BlockSpec(memory_space=pltpu.VMEM),
        ],
        out_specs=pl.BlockSpec(memory_space=pl.ANY),
        out_shape=jax.ShapeDtypeStruct((fields, tiles * tile_cells), jnp.float32),
        scratch_shapes=[
            pltpu.VMEM((fields, (tiles + 1) * tile_cells), jnp.float32),
            pltpu.VMEM((tiles, tile_cells), jnp.float32),
            pltpu.VMEM((8, 128), jnp.int32),
            pltpu.SMEM((8, 128), jnp.int32),
            pltpu.SMEM((X * CAP * planes * R + 8,), jnp.int32),
            pltpu.SemaphoreType.DMA,
            pltpu.SemaphoreType.DMA,
        ],
        compiler_params=pltpu.CompilerParams(vmem_limit_bytes=24 << 20),
        name="place",
    )(near.reshape(-1, ROWS, tile_cells), far.reshape(-1, ROWS, tile_cells), ocean_mask.reshape(tiles, tile_cells))


def solution(mesh):
    in_specs = (
        P(None, ("band", "sub")),
        P(("band", "sub"), None, None),
        P(("band", "sub")),
        P(("band", "sub"), None),
        P(("band", "sub")),
        P(("band", "sub")),
    )
    return jax.shard_map(
        per_device, mesh=mesh, in_specs=in_specs, out_specs=P(None, ("band", "sub")), check_vma=False
    )
```

```python
import functools

import jax
import jax.numpy as jnp
from jax import lax
from jax.experimental import pallas as pl
from jax.experimental.pallas import tpu as pltpu
from jax.sharding import PartitionSpec as P

cover_floor = 0.5
MESH = pl.DeviceIdType.MESH
CAP = 2
XLO = 2
X = 4
R = 8
ROWS = 8
CODE = 32


def place():
    band, sub = lax.axis_index("band"), lax.axis_index("sub")
    z, x_lo, rem = band // (XLO * R), (band // R) % XLO, band % R
    return z, x_lo, rem, sub * XLO + x_lo


def make_table(band_ref, tile_ref, out_ref):
    blocks = band_ref.shape[1]
    down = lax.broadcasted_iota(jnp.int32, (blocks, blocks), 0)
    across = lax.broadcasted_iota(jnp.int32, (blocks, blocks), 1)
    out_ref[...] = jnp.zeros_like(out_ref)
    band = jnp.broadcast_to(band_ref[...], (blocks, blocks))
    tile = jnp.broadcast_to(tile_ref[...], (blocks, blocks))
    band_down = jnp.sum(jnp.where(down == across, band, 0), axis=1, keepdims=True)
    tile_down = jnp.sum(jnp.where(down == across, tile, 0), axis=1, keepdims=True) + 1
    rank_down = jnp.sum(jnp.where((band == band_down) & (across < down), 1, 0), axis=1, keepdims=True)
    slot_down = band_down * CAP + rank_down
    for part in range(CAP):
        here = slot_down == across + part * blocks
        for row, value in enumerate((down, tile_down // CODE, tile_down % CODE)):
            out_ref[row : row + 1, part * blocks : (part + 1) * blocks] = jnp.sum(
                jnp.where(here, value, 0), axis=0, keepdims=True
            )


SOURCES = ((0, 0), (0, 1), (1, 0), (-1, 0), (1, 1), (-1, 1), (2, 0), (2, 1))
HOPS = [(far, hop) for far in range(1, 5) for hop in range(1, far + 1)]


def exchange_kernel(
    pieces, band_hbm, tile_hbm, values_hbm, weights_hbm, mask_hbm, near_ref, far_ref,
    band_ref, tile_ref, table_vmem, table_ref, values_ref, weights_ref, mask_ref, in_sem, stage, held, relay, y_send, y_recv, z_send, z_recv, x_send, x_recv,
):
    names = [
        pltpu.make_async_copy(band_hbm, band_ref, in_sem.at[3]),
        pltpu.make_async_copy(tile_hbm, tile_ref, in_sem.at[4]),
    ]
    loads = [
        pltpu.make_async_copy(weights_hbm, weights_ref, in_sem.at[1]),
        pltpu.make_async_copy(mask_hbm, mask_ref, in_sem.at[2]),
    ]
    for load in names + loads:
        load.start()

    def load_block(block, _):
        cells = pl.ds(pl.multiple_of(block * 128, 128), 128)
        pltpu.make_async_copy(values_hbm.at[:, cells], values_ref.at[block], in_sem.at[0]).start()
        return 0

    lax.fori_loop(0, values_ref.shape[0], load_block, 0)
    loads.append(pltpu.make_async_copy(values_ref, values_ref, in_sem.at[0]))
    half = CAP * pieces + 1
    planes = near_ref.shape[0]
    fields = values_ref.shape[1]
    z, x_lo, rem, x = place()
    y, core = rem // 2, rem % 2
    ring_y = R // 2
    row = lax.broadcasted_iota(jnp.int32, (ROWS, 128), 0)
    lane = lax.broadcasted_iota(jnp.int32, (ROWS, 128), 1)

    def device(z_to=z, rem_to=rem, x_to=x):
        return {"band": z_to * (XLO * R) + (x_to % XLO) * R + rem_to, "sub": x_to // XLO}

    def mate(index, sign):
        dy, dc = SOURCES[index]
        return ((y + ring_y + sign * dy) % ring_y) * 2 + (core + dc) % 2

    def fill(unit, ahead, to):
        start = ahead * R + rem
        sides = jnp.zeros((ROWS, 128), jnp.float32)
        for part in range(2):
            lo = x_lo if part == 0 else XLO - 1 - x_lo
            slot = (((z + ahead) % planes) * (XLO * R) + lo * R + to) * CAP
            for rank in range(CAP):
                block = table_ref[0, slot + rank]
                keep = mask_ref[block].astype(jnp.float32).astype(jnp.bfloat16)
                left = values_ref[block] * keep
                left = jnp.concatenate([left, jnp.broadcast_to(keep, (16, 128))], axis=0)
                product = jnp.dot(left, weights_ref[block], preferred_element_type=jnp.float32)
                first = part * half + rank * pieces
                unit[first : first + pieces] = product[:fields].reshape(pieces, ROWS, 128).astype(jnp.bfloat16)
                sides = jnp.where(row == part * CAP + rank, product[fields : fields + ROWS], sides)
                for digit in range(2):
                    here = (row == 4 + part * 2 + digit) & (lane == start + rank * planes * R)
                    sides = jnp.where(here, table_ref[1 + digit, slot + rank].astype(jnp.float32), sides)
        unit[half - 1] = sides.astype(jnp.bfloat16)

    def prepare(i):
        to = mate(i, 1)

        def one(ahead, _):
            fill(stage.at[i, ahead], ahead, to)
            return 0

        lax.fori_loop(1, planes, one, 0)

    right, left = (z + 1) % planes, (z + planes - 1) % planes
    ways = (1, X - 1, 2)

    barrier = pltpu.get_barrier_semaphore()
    greeted = [device(rem_to=mate(i, 1)) for i in range(1, R)] + [device(z_to=right), device(z_to=left)]
    greeted += [device(x_to=(x + shift) % X) for shift in ways]
    for peer in greeted:
        pl.semaphore_signal(barrier, inc=1, device_id=peer, device_id_type=MESH)
    for load in names:
        load.wait()
    make_table(band_ref, tile_ref, table_vmem)
    loads.append(pltpu.make_async_copy(table_vmem, table_ref, in_sem.at[5]))
    loads[-1].start()
    for load in loads:
        load.wait()
    fill(near_ref.at[0, rem], 0, rem)
    for i in range(1, R):
        fill(stage.at[i, 0], 0, mate(i, 1))
    prepare(0)
    pl.semaphore_wait(barrier, len(greeted))

    def remote(src, dst, send_sem, recv_sem, peer):
        return pltpu.make_async_remote_copy(
            src_ref=src, dst_ref=dst, send_sem=send_sem, recv_sem=recv_sem, device_id=peer, device_id_type=MESH
        )

    def y_copy(i, onward):
        to = mate(i, 1)
        src = stage.at[i, pl.ds(1, planes - 1)] if onward else stage.at[i, 0]
        dst = held.at[:, rem] if onward else near_ref.at[0, rem]
        return remote(src, dst, y_send.at[onward, i], y_recv.at[onward, i], device(rem_to=to))

    def forward(ahead, source):
        for way, shift in reversed(list(enumerate(ways))):
            begin = half - 1 if way < 2 else 0
            remote(
                near_ref.at[ahead, source, pl.ds(begin, half)],
                far_ref.at[way, ahead, source],
                x_send.at[way],
                x_recv.at[way],
                device(x_to=(x + shift) % X),
            ).start()

    def travels(i, way, far):
        return far < 4 or i % 2 == way

    def z_copy(i, way, far, hop):
        source = mate(i, -1)
        at = far if way == 0 else planes - far
        slot = (far - 1) * (far - 2) // 2
        first = stage.at[0, at] if i == 0 else held.at[at - 1, source]
        src = first if hop == 1 else relay.at[way, i, slot + hop - 2]
        dst = near_ref.at[at, source] if hop == far else relay.at[way, i, slot + hop - 1]
        sem = z_recv.at[way, i, HOPS.index((far, hop))]
        return remote(src, dst, z_send.at[way], sem, device(z_to=right if way == 0 else left))

    def arrive(i, way, far, hop):
        z_copy(i, way, far, hop).wait_recv()
        if hop == far:
            forward(far if way == 0 else planes - far, mate(i, -1))
        else:
            z_copy(i, way, far, hop + 1).start()

    def own_plane(i):
        y_copy(i, 0).wait_recv()
        forward(0, mate(i, -1))

    computed = {0: (2, 1, 3), 1: (4, 5), 3: (6, 7)}
    sent = {0: (2, 1, 3), 2: (4, 5), 4: (6,), 5: (7,)}

    def arrivals(turn):
        for hop in (1, 2, 3, 4):
            i = turn - hop
            if 0 <= i < R:
                for far in range(hop, 5):
                    for way in (0, 1):
                        if travels(i, way, far):
                            arrive(i, way, far, hop)

    for turn in range(R + 4):
        if turn == 2:
            arrivals(turn)
        if turn < R:
            if turn > 0:
                y_copy(turn, 1).wait_recv()
            for far in (1, 2, 3, 4):
                for way in (0, 1):
                    if travels(turn, way, far):
                        z_copy(turn, way, far, 1).start()
        if turn == 0:
            for i in range(1, R):
                y_copy(i, 0).start()
            forward(0, rem)
        if turn == 1:
            for i in range(1, R):
                own_plane(i)
        for i in computed.get(turn, ()):
            prepare(i)
            if i in sent.get(turn, ()):
                y_copy(i, 1).start()
        for i in sent.get(turn, ()):
            if i not in computed.get(turn, ()):
                y_copy(i - 2, 1).wait_send()
                y_copy(i, 1).start()
        if turn != 2:
            arrivals(turn)

    for i in range(1, R):
        y_copy(i, 0).wait_send()
        if i not in (2, 3, 4, 5):
            y_copy(i, 1).wait_send()
    for way in (0, 1):
        remote(near_ref, near_ref, z_send.at[way], y_recv.at[0, 0], device()).wait_send()
    for way in range(X - 1):
        remote(far_ref.at[way], far_ref.at[way], x_send.at[way], x_recv.at[way], device()).wait()


def place_kernel(
    pieces, planes, near_ref, far_ref, ocean_ref, out_ref,
    total, scale, codes, code_smem, picked, code_sem, out_sem,
):
    half = CAP * pieces + 1
    tiles = ocean_ref.shape[0]
    sources = planes * R
    sub = lax.axis_index("sub")

    tile_down = lax.broadcasted_iota(jnp.int32, (tiles, sources), 0) + sub * tiles
    cover = jnp.zeros((tiles, 128), jnp.float32)
    for part in range(X):
        other = part in (1, 2)
        if part == 0:
            sides = near_ref.reshape(sources, 2 * half - 1, ROWS, 128)[:, half - 1]
        else:
            sides = far_ref.reshape(X - 1, sources, half, ROWS, 128)[part - 1, :, 0 if other else half - 1]
        sides = sides.astype(jnp.float32)
        digits = jnp.sum(sides, axis=0)
        digit = 6 if other else 4
        number = (digits[digit : digit + 1] * CODE + digits[digit + 1 : digit + 2]).astype(jnp.int32) - 1
        codes[part : part + 1, :] = number
        for rank in range(CAP):
            row = rank + (CAP if other else 0)
            chosen = tile_down == number[:, rank * sources : (rank + 1) * sources]
            chosen = jnp.where(chosen, 1.0, 0.0).astype(jnp.bfloat16)
            cover += jnp.dot(chosen, sides[:, row].astype(jnp.bfloat16), preferred_element_type=jnp.float32)
    copy = pltpu.make_async_copy(codes, code_smem, code_sem)
    copy.start()
    scale[...] = ocean_ref[...].astype(jnp.float32) / jnp.maximum(cover, cover_floor)

    def clear(i, _):
        total[:, pl.ds(pl.multiple_of(i * 1280, 128), 1280)] = jnp.zeros((total.shape[0], 1280), jnp.float32)
        return 0

    lax.fori_loop(0, tiles // 10, clear, 0)
    copy.wait()

    def pick(part, stride, offset, count):
        for rank in range(CAP):

            def one(step, count, rank=rank):
                for k in range(8):
                    source = step * 8 + k
                    tile = code_smem[part, rank * sources + source] - sub * tiles
                    start = offset + source * stride + rank * pieces
                    picked[count] = start * 256 + tile
                    count = count + jnp.where((tile >= 0) & (tile < tiles), 1, 0)
                return count

            count = lax.fori_loop(0, sources // 8, one, count)
        return count

    def add(ref, count):
        group = 4
        for k in range(group):
            picked[count + k] = tiles

        def several(step, _):
            slots = []
            for k in range(group):
                entry = picked[step * group + k]
                slot = ref[pl.ds(entry // 256, pieces)].astype(jnp.float32).reshape(pieces * ROWS, 128)
                slots.append((pl.ds(pl.multiple_of((entry % 256) * 128, 128), 128), slot))
            for cells, slot in slots:
                total[:, cells] += slot
            return 0

        lax.fori_loop(0, (count + group - 1) // group, several, 0)

    add(near_ref, pick(0, 2 * half - 1, 0, 0))
    count = pick(1, half, 1, 0)
    count = pick(2, half, sources * half + 1, count)
    add(far_ref, pick(3, half, 2 * sources * half, count))

    group = 8

    def finish(i, _):
        for k in range(group):
            tile = i * group + k
            cells = pl.ds(pl.multiple_of(tile * 128, 128), 128)
            total[:, cells] = total[:, cells] * scale[pl.ds(tile, 1), :]
        cells = pl.ds(pl.multiple_of(i * group * 128, 128), group * 128)
        pltpu.make_async_copy(total.at[:, cells], out_ref.at[:, cells], out_sem).start()
        return 0

    lax.fori_loop(0, tiles // group, finish, 0)
    pltpu.make_async_copy(total.at[:, pl.ds(0, tiles * 128)], out_ref, out_sem).wait()


def per_device(land_values, area_weights, land_mask, dest_band, dest_tile, ocean_mask):
    fields = land_values.shape[0]
    blocks, cells, tile_cells = area_weights.shape
    bands = lax.axis_size("band")
    planes = bands // (XLO * R)
    pieces = fields // ROWS
    half = CAP * pieces + 1
    tiles = ocean_mask.shape[0] // tile_cells
    unit = (2 * half - 1, ROWS, tile_cells)
    near, far = pl.pallas_call(
        functools.partial(exchange_kernel, pieces),
        in_specs=[pl.BlockSpec(memory_space=pltpu.HBM)] * 5,
        out_specs=[pl.BlockSpec(memory_space=pltpu.VMEM)] * 2,
        out_shape=[
            pltpu.VMEM((planes, R, *unit), jnp.bfloat16),
            pltpu.VMEM((X - 1, planes, R, half, ROWS, tile_cells), jnp.bfloat16),
        ],
        scratch_shapes=[
            pltpu.VMEM((1, blocks), jnp.int32),
            pltpu.VMEM((1, blocks), jnp.int32),
            pltpu.VMEM((8, bands * CAP), jnp.int32),
            pltpu.SMEM((8, bands * CAP), jnp.int32),
            pltpu.VMEM((blocks, fields, cells), jnp.bfloat16),
            pltpu.VMEM(area_weights.shape, jnp.bfloat16),
            pltpu.VMEM((blocks, 1, cells), jnp.int32),
            pltpu.SemaphoreType.DMA((6,)),
            pltpu.VMEM((R, planes, *unit), jnp.bfloat16),
            pltpu.VMEM((planes - 1, R, *unit), jnp.bfloat16),
            pltpu.VMEM((2, R, 6, *unit), jnp.bfloat16),
            pltpu.SemaphoreType.DMA((2, R)),
            pltpu.SemaphoreType.DMA((2, R)),
            pltpu.SemaphoreType.DMA((2,)),
            pltpu.SemaphoreType.DMA((2, R, len(HOPS))),
            pltpu.SemaphoreType.DMA((X - 1,)),
            pltpu.SemaphoreType.DMA((X - 1,)),
        ],
        compiler_params=pltpu.CompilerParams(collective_id=0, has_side_effects=True, vmem_limit_bytes=50 << 20),
        name="exchange",
    )(
        dest_band.reshape(1, blocks),
        dest_tile.reshape(1, blocks),
        land_values,
        area_weights,
        land_mask.reshape(blocks, 1, cells),
    )
    near, far = near.reshape(planes * R, *unit), far.reshape(X - 1, planes * R, half, ROWS, tile_cells)
    return pl.pallas_call(
        functools.partial(place_kernel, pieces, planes),
        in_specs=[
            pl.BlockSpec(memory_space=pltpu.VMEM),
            pl.BlockSpec(memory_space=pltpu.VMEM),
            pl.BlockSpec(memory_space=pltpu.VMEM),
        ],
        out_specs=pl.BlockSpec(memory_space=pl.ANY),
        out_shape=jax.ShapeDtypeStruct((fields, tiles * tile_cells), jnp.float32),
        scratch_shapes=[
            pltpu.VMEM((fields, (tiles + 1) * tile_cells), jnp.float32),
            pltpu.VMEM((tiles, tile_cells), jnp.float32),
            pltpu.VMEM((8, 128), jnp.int32),
            pltpu.SMEM((8, 128), jnp.int32),
            pltpu.SMEM((X * CAP * planes * R + 8,), jnp.int32),
            pltpu.SemaphoreType.DMA,
            pltpu.SemaphoreType.DMA,
        ],
        compiler_params=pltpu.CompilerParams(vmem_limit_bytes=24 << 20),
        name="place",
    )(near.reshape(-1, ROWS, tile_cells), far.reshape(-1, ROWS, tile_cells), ocean_mask.reshape(tiles, tile_cells))


def solution(mesh):
    in_specs = (
        P(None, ("band", "sub")),
        P(("band", "sub"), None, None),
        P(("band", "sub")),
        P(("band", "sub"), None),
        P(("band", "sub")),
        P(("band", "sub")),
    )
    return jax.shard_map(
        per_device, mesh=mesh, in_specs=in_specs, out_specs=P(None, ("band", "sub")), check_vma=False
    )
```
